32 devices in a mesh: ctx: 8 (over z, y), sub: 4 (over x, core).
Axes of the slice: x: 2, y: 2, z: 4, core: 2. Of those that a mesh axis runs over, the one named last changes fastest.
Arguments:
- queries: float32 [64, 128, 512], P('ctx', 'sub'), may hold values from -128 to 128
- keys: float32 [8, 1024, 256], P('ctx', 'sub'), may hold values from -8 to 8
- values: float32 [8, 1024, 256], P('ctx', 'sub'), may hold values from -6 to 6
- selected: int32 [64, 2, 3], P('ctx'), may hold values from 0 to 8, as said below
Outputs:
- attended: float32 [64, 128, 512], P('ctx', 'sub')
The draws below stay inside these ranges and needn't reach their ends.
Inputs may be any that keep to these rules, and one draw needn't show every extreme that they name: `selected`: within a row the entries below the tile's own block are distinct. Within each head group, each block is named by at most one tile of each aligned run of 8 tiles. Over all head groups, each aligned run of 8 tiles names at most 1 distinct (block, group) pairs among the blocks of any one aligned run of 1 block, and some run reaches 1 in every draw. Entries that are not below the own block equal 8.
All inputs are finite; a program needn't handle non-finite values.
Results may differ from the reference program's by a relative error of at most 0.0003.
Values sent between devices are 32-bit elements; how exact they have to be, the bound alone decides.
No kernel may reach another device: no remote copies, remote signals or barrier semaphores. Data moves between devices by JAX's collectives and lax.ppermute only.
A program may use at most 64 MiB of HBM per device.

```python
import jax
import jax.numpy as jnp
from jax import lax

QUERY_HEADS = 4
KEY_VALUE_HEADS = 2
HEAD_SIZE = 128
TILE = 128
BLOCK_KEYS = 1024
CHOSEN_BLOCKS = 3
TILES_PER_SHARD = 8
BLOCKS_PER_SHARD = 1
SLOTS = 1
QUERY_TILES = 64
WINDOW_BLOCKS = 8


def shared_fields(key):
    query_key = jax.random.fold_in(key, 11)
    key_random_seed = jax.random.fold_in(key, 12)
    query_field = jax.random.truncated_normal(query_key, -6.0, 6.0, (QUERY_TILES, TILE, QUERY_HEADS * HEAD_SIZE), jnp.float32)
    key_tensor = jax.random.truncated_normal(key_random_seed, -6.0, 6.0, (WINDOW_BLOCKS, BLOCK_KEYS, KEY_VALUE_HEADS * HEAD_SIZE), jnp.float32)
    query_field = jnp.clip(query_field, -128.0, 128.0)
    key_tensor = jnp.clip(key_tensor, -8.0, 8.0)
    return (query_field, key_tensor)


def draw_queries(key, part):
    return shared_fields(key)[0]


def draw_keys(key, part):
    return shared_fields(key)[1]


def draw_selected(key, part):
    repeat_runs = QUERY_TILES // TILES_PER_SHARD
    pairing_total = KEY_VALUE_HEADS * BLOCKS_PER_SHARD
    selection_total = TILES_PER_SHARD * CHOSEN_BLOCKS
    feature_width = min(selection_total, WINDOW_BLOCKS)
    pair_key = jax.random.fold_in(key, 21)
    jitter_seed = jax.random.fold_in(key, 22)
    pair_scores = jax.random.randint(pair_key, (repeat_runs, repeat_runs, pairing_total), 0, 4096) * pairing_total + jnp.arange(pairing_total, dtype=jnp.int32)
    order = jnp.argsort(pair_scores, axis=2)
    ranks = jnp.argsort(order, axis=2)
    allowed_mask = ranks < SLOTS
    run_ids = jnp.arange(repeat_runs, dtype=jnp.int32)
    allowed_mask = allowed_mask & (run_ids[None, :, None] < run_ids[:, None, None])
    allowed_mask = allowed_mask.reshape(repeat_runs, repeat_runs, BLOCKS_PER_SHARD, KEY_VALUE_HEADS).transpose(0, 3, 1, 2).reshape(repeat_runs, KEY_VALUE_HEADS, WINDOW_BLOCKS)
    block_ids = jnp.arange(WINDOW_BLOCKS, dtype=jnp.int32)
    random_jitter = jax.random.randint(jitter_seed, (repeat_runs, KEY_VALUE_HEADS, WINDOW_BLOCKS), 0, 4096)
    score = (allowed_mask.astype(jnp.int32) * 4096 + random_jitter) * WINDOW_BLOCKS + block_ids
    picked = lax.top_k(score, feature_width)[1].astype(jnp.int32)
    valid = jnp.take_along_axis(allowed_mask, picked, axis=2)
    table_entries = jnp.where(valid, picked, WINDOW_BLOCKS).astype(jnp.int32)
    if feature_width < selection_total:
        table_entries = jnp.concatenate([table_entries, jnp.full((repeat_runs, KEY_VALUE_HEADS, selection_total - feature_width), WINDOW_BLOCKS, jnp.int32)], axis=2)
    table_entries = table_entries.reshape(repeat_runs, KEY_VALUE_HEADS, TILES_PER_SHARD, CHOSEN_BLOCKS).transpose(0, 2, 1, 3).reshape(QUERY_TILES, KEY_VALUE_HEADS, CHOSEN_BLOCKS)
    return table_entries.astype(jnp.int32)


def block_levels(rng, shape, split, least, high):
    loudness, own = 1.0, jax.random.fold_in(rng, 6)
    for axis_at, blocks in split:
        draws = jnp.exp(jax.random.uniform(jax.random.fold_in(own, axis_at), (blocks,), jnp.float32, least / len(split), high / len(split)))
        loudness = loudness * jnp.repeat(draws, shape[axis_at] // blocks).reshape([-1 if axis == axis_at else 1 for axis in range(len(shape))])
    return loudness


def noise(own_key, shape, spread, reach, split=(), held_as=jnp.bfloat16):
    level = block_levels(own_key, shape, split, -0.22, 0.18) if split else 1.0
    entries = jax.random.normal(own_key, shape, jnp.float32) * spread * level
    return jnp.minimum(jnp.maximum(entries, -reach), reach).astype(held_as)


def setup_inputs(seed: int = 0) -> dict:
    seeds = jax.random.split(jax.random.key(seed), 5)
    queries = draw_queries(jax.random.fold_in(seeds[4], 71), 0)
    keys = draw_keys(jax.random.fold_in(seeds[4], 71), 0)
    values = noise(seeds[2], (WINDOW_BLOCKS, BLOCK_KEYS, KEY_VALUE_HEADS * HEAD_SIZE), 1.0, 6.0, ((0, 8), (1, 4)), jnp.float32)
    selected = draw_selected(jax.random.fold_in(seeds[4], 71), 0)
    return {"queries": queries, "keys": keys, "values": values, "selected": selected}


highest = lax.Precision.HIGHEST


def reference(queries, keys, values, selected):
    tile_total, tile_row_span, full_width = queries.shape
    block_grand_total, block_row_span, kv_width = keys.shape
    each_block = block_row_span // tile_row_span
    group_extent = QUERY_HEADS // KEY_VALUE_HEADS
    key_head_rows = keys.reshape(block_grand_total, block_row_span, KEY_VALUE_HEADS, HEAD_SIZE)
    value_head_rows = values.reshape(block_grand_total, block_row_span, KEY_VALUE_HEADS, HEAD_SIZE)

    def single(tile_identifier):
        query_tile_rows = lax.dynamic_index_in_dim(queries, tile_identifier, 0, keepdims=False).reshape(tile_row_span, KEY_VALUE_HEADS, group_extent, HEAD_SIZE)
        own_block = tile_identifier // each_block
        limits = (tile_identifier % each_block) * tile_row_span + jnp.arange(tile_row_span, dtype=jnp.int32)
        own_keys = lax.dynamic_index_in_dim(key_head_rows, own_block, 0, keepdims=False)
        own_values = lax.dynamic_index_in_dim(value_head_rows, own_block, 0, keepdims=False)
        choice_row = lax.dynamic_index_in_dim(selected, tile_identifier, 0, keepdims=False)
        visible = choice_row < own_block
        outputs = []
        for group_position in range(KEY_VALUE_HEADS):
            clamped = jnp.where(visible[group_position], choice_row[group_position], 0).astype(jnp.int32)
            chosen_keys = key_head_rows[clamped, :, group_position].reshape(CHOSEN_BLOCKS * block_row_span, HEAD_SIZE)
            chosen_values = value_head_rows[clamped, :, group_position].reshape(CHOSEN_BLOCKS * block_row_span, HEAD_SIZE)
            all_keys = jnp.concatenate([chosen_keys, own_keys[:, group_position]], axis=0)
            all_values = jnp.concatenate([chosen_values, own_values[:, group_position]], axis=0)
            mask_chosen = jnp.repeat(visible[group_position], block_row_span, total_repeat_length=CHOSEN_BLOCKS * block_row_span)
            mask_own = jnp.arange(block_row_span, dtype=jnp.int32)[None, :] <= limits[:, None]
            allowed = jnp.concatenate([jnp.broadcast_to(mask_chosen[None, :], (tile_row_span, CHOSEN_BLOCKS * block_row_span)), mask_own], axis=1)
            scores = jnp.einsum("qhd,kd->hqk", query_tile_rows[:, group_position], all_keys, precision=highest) * (HEAD_SIZE ** -0.5)
            scores = jnp.where(allowed[None], scores, -jnp.inf)
            weights = jax.nn.softmax(scores, axis=-1)
            outputs.append(jnp.einsum("hqk,kd->qhd", weights, all_values, precision=highest))
        return jnp.stack(outputs, axis=1).reshape(tile_row_span, full_width)

    return lax.map(single, jnp.arange(tile_total, dtype=jnp.int32))
```

```python
import functools
import math

import jax
import jax.numpy as jnp
from jax import lax
from jax.experimental import pallas as pl
from jax.experimental.pallas import tpu as pltpu
from jax.sharding import PartitionSpec as P

QUERY_HEADS = 4
KEY_VALUE_HEADS = 2
HEAD_SIZE = 128
GROUP = QUERY_HEADS // KEY_VALUE_HEADS
CORES = 2
LANES = 128
PAD = 8

LOW_FILL = -1e30
SCALE = HEAD_SIZE ** (-0.5) * math.log2(math.e)


VMEM = pl.BlockSpec(memory_space=pltpu.VMEM)
SMEM = pl.BlockSpec(memory_space=pltpu.SMEM)
PARAMS = pltpu.CompilerParams(vmem_limit_bytes=24 * 1024 * 1024)


def halves(x):
    high = x.astype(jnp.bfloat16)
    low = (x - high.astype(jnp.float32)).astype(jnp.bfloat16)
    return high, low


def dot_nt(a, b):
    return lax.dot_general(
        a, b, (((1,), (1,)), ((), ())), preferred_element_type=jnp.float32
    )


def dot_nn(a, b):
    return lax.dot_general(
        a, b, (((1,), (0,)), ((), ())), preferred_element_type=jnp.float32
    )


def pack_kernel(place_ref, sel_ref, q_ref, packed_ref, route_ref):
    tiles, rows, _ = q_ref.shape
    shards, span, _ = packed_ref.shape
    picks = sel_ref.shape[2]
    mine = place_ref[0]
    packed_ref[...] = jnp.zeros_like(packed_ref)
    for d in range(shards):
        route_ref[d] = -1

    def visit(t, carry):
        for g in range(KEY_VALUE_HEADS):
            for c in range(picks):
                d = sel_ref[t, g, c]

                @pl.when(d < mine)
                def _():
                    route_ref[d] = t * KEY_VALUE_HEADS + g
                    for h in range(GROUP):
                        column = (g * GROUP + h) * HEAD_SIZE
                        packed_ref[d, h * rows : (h + 1) * rows, :] = (
                            q_ref[t, :, column : column + HEAD_SIZE] * SCALE
                        )
                    packed_ref[d, GROUP * rows : span, :] = jnp.full(
                        (PAD, LANES), g, jnp.float32
                    )

        return carry

    lax.fori_loop(0, tiles, visit, 0)


def own_scores(place_ref, offsets, q_ref, k_refs, head_pair):
    tiles, rows, _ = q_ref.shape
    per_head = tiles * rows
    key_rows = k_refs[0].shape[0]
    sub = place_ref[1]
    tile_span = rows * place_ref[2]
    q = jnp.concatenate(
        [
            q_ref[:, :, (head_pair * GROUP + h) * HEAD_SIZE : (head_pair * GROUP + h + 1) * HEAD_SIZE]
            .reshape(per_head, HEAD_SIZE)
            for h in range(GROUP)
        ],
        axis=0,
    )
    high, low = halves(q * SCALE)
    left = jnp.concatenate([high, low, high, low], axis=1)
    row = lax.broadcasted_iota(jnp.int32, (GROUP * per_head, key_rows), 0) % per_head
    row = row // rows * tile_span + row % rows + sub * rows
    column = lax.broadcasted_iota(jnp.int32, (GROUP * per_head, key_rows), 1)
    gap = column - row
    pieces = []
    for k_ref, offset in zip(k_refs, offsets):
        k_high, k_low = halves(k_ref[:, head_pair * HEAD_SIZE : (head_pair + 1) * HEAD_SIZE])
        right = jnp.concatenate([k_high, k_high, k_low, k_low], axis=1)
        score = dot_nt(left, right)
        pieces.append(jnp.where(gap <= -offset * key_rows, score, LOW_FILL))
    return pieces


def row_max(pieces):
    top = pieces[0]
    for piece in pieces[1:]:
        top = jnp.maximum(top, piece)
    return jnp.max(top, axis=1, keepdims=True)


def row_sum(pieces):
    total = pieces[0]
    for piece in pieces[1:]:
        total = total + piece
    return jnp.sum(total, axis=1, keepdims=True)


def own_values(weights, v_refs, head_pair):
    total = None
    for weight, v_ref in zip(weights, v_refs):
        w_high, w_low = halves(weight)
        v_high, v_low = halves(v_ref[:, head_pair * HEAD_SIZE : (head_pair + 1) * HEAD_SIZE])
        right = jnp.concatenate([v_high, v_low], axis=1)
        part = dot_nn(w_high, right) + dot_nn(w_low, right)
        total = part if total is None else total + part
    return total[:, :HEAD_SIZE] + total[:, HEAD_SIZE:]


def own_kernel(first, last, count, place_ref, offsets_ref, q_ref, *refs):
    k_refs, v_refs, rest = refs[:count], refs[count : 2 * count], refs[2 * count :]
    tiles, rows, _ = q_ref.shape
    per_head = tiles * rows
    offsets = [offsets_ref[i] for i in range(count)]
    for g in range(KEY_VALUE_HEADS):
        span = pl.ds(g * GROUP * per_head, GROUP * per_head)
        pieces = own_scores(place_ref, offsets, q_ref, k_refs, g)
        top = row_max(pieces)
        if not first:
            max_ref, sum_ref, acc_ref = rest[:3]
            before = max_ref[span, :1]
            top = jnp.maximum(top, before)
        weights = [jnp.exp2(piece - top) for piece in pieces]
        total = row_sum(weights)
        acc = own_values(weights, v_refs, g)
        if not first:
            shrink = jnp.exp2(before - top)
            total = total + shrink * sum_ref[span, :1]
            acc = acc + shrink * acc_ref[span, :]
        if last:
            out_ref, lse_ref = rest[-2:]
            out = acc / total
            for h in range(GROUP):
                column = (g * GROUP + h) * HEAD_SIZE
                out_ref[:, :, column : column + HEAD_SIZE] = out[
                    h * per_head : (h + 1) * per_head
                ].reshape(tiles, rows, HEAD_SIZE)
            lse_ref[span, :] = jnp.broadcast_to(top + jnp.log2(total), acc.shape)
        else:
            max_out, sum_out, acc_out = rest[-3:]
            max_out[span, :] = jnp.broadcast_to(top, acc.shape)
            sum_out[span, :] = jnp.broadcast_to(total, acc.shape)
            acc_out[span, :] = acc


def own_pass(first, last, place, offsets, queries, keys, values, state):
    tiles, rows, width = queries.shape
    count = len(keys)
    state_shape = jax.ShapeDtypeStruct((tiles * rows * QUERY_HEADS, LANES), jnp.float32)
    if last:
        out_shape = (jax.ShapeDtypeStruct(queries.shape, jnp.float32), state_shape)
    else:
        out_shape = (state_shape,) * 3
    return pl.pallas_call(
        functools.partial(own_kernel, first, last, count),
        out_shape=out_shape,
        in_specs=[SMEM, SMEM] + [VMEM] * (1 + 2 * count + len(state)),
        out_specs=tuple([VMEM] * len(out_shape)),
        compiler_params=PARAMS,
        name="own_last" if last else "own_first",
    )(place, offsets, queries, *keys, *values, *state)


def routed_kernel(first, last, count, packed_ref, *refs):
    k_refs, v_refs, rest = refs[:count], refs[count : 2 * count], refs[2 * count :]
    shards, span, _ = packed_ref.shape
    body = span - PAD
    total_rows = shards * body
    label = jnp.broadcast_to(packed_ref[:, body : body + 1, :], (shards, body, LANES)).reshape(
        total_rows, LANES
    )
    rows = packed_ref[:, :body, :].reshape(total_rows, HEAD_SIZE)
    wide = jnp.concatenate(
        [jnp.where(label == g, rows, 0.0) for g in range(KEY_VALUE_HEADS)], axis=1
    )
    high, low = halves(wide)
    left = jnp.concatenate([high, low, high], axis=1)
    pieces = []
    for k_ref in k_refs:
        k_high, k_low = halves(k_ref[...])
        pieces.append(dot_nt(left, jnp.concatenate([k_high, k_high, k_low], axis=1)))
    top = row_max(pieces)
    if not first:
        max_ref, sum_ref, acc_ref = rest[:3]
        before = max_ref[:, :1]
        top = jnp.maximum(top, before)
    weights = [jnp.exp2(piece - top) for piece in pieces]
    total = row_sum(weights)
    result = None
    for weight, v_ref in zip(weights, v_refs):
        w_high, w_low = halves(weight)
        v_high, v_low = halves(v_ref[...])
        part = dot_nn(w_high, v_high) + dot_nn(w_low, v_high) + dot_nn(w_high, v_low)
        result = part if result is None else result + part
    acc = result[:, :HEAD_SIZE]
    for g in range(1, KEY_VALUE_HEADS):
        acc = jnp.where(label == g, result[:, g * HEAD_SIZE : (g + 1) * HEAD_SIZE], acc)
    if not first:
        shrink = jnp.exp2(before - top)
        total = total + shrink * sum_ref[:, :1]
        acc = acc + shrink * acc_ref[...]
    if last:
        reply_ref = rest[-1]
        reply_ref[:, :body, :] = (acc / total).reshape(shards, body, HEAD_SIZE)
        lse = jnp.broadcast_to(top + jnp.log2(total), (total_rows, LANES)).reshape(
            shards, body, LANES
        )
        row = lax.broadcasted_iota(jnp.int32, (shards, body, LANES), 1)
        lane = lax.broadcasted_iota(jnp.int32, (shards, body, LANES), 2)
        line = jnp.sum(jnp.where(row == lane, lse, 0.0), axis=1, keepdims=True)
        reply_ref[:, body:, :] = jnp.broadcast_to(line, (shards, PAD, LANES))
    else:
        max_out, sum_out, acc_out = rest[-3:]
        max_out[...] = jnp.broadcast_to(top, acc.shape)
        sum_out[...] = jnp.broadcast_to(total, acc.shape)
        acc_out[...] = acc


def routed_pass(first, last, packed, keys, values, state):
    shards, span, _ = packed.shape
    count = len(keys)
    state_shape = jax.ShapeDtypeStruct((shards * (span - PAD), LANES), jnp.float32)
    if last:
        out_shape = (jax.ShapeDtypeStruct(packed.shape, jnp.float32),)
    else:
        out_shape = (state_shape,) * 3
    return pl.pallas_call(
        functools.partial(routed_kernel, first, last, count),
        out_shape=out_shape,
        in_specs=[VMEM] * (1 + 2 * count + len(state)),
        out_specs=tuple([VMEM] * len(out_shape)),
        compiler_params=PARAMS,
        name="routed_last" if last else "routed_first",
    )(packed, *keys, *values, *state)


def merge_kernel(route_ref, reply_ref, own_ref, lse_ref, out_ref, run_ref):
    tiles, rows, _ = own_ref.shape
    shards, span, _ = reply_ref.shape
    body = span - PAD
    out_ref[...] = own_ref[...]
    run_ref[...] = lse_ref[...]
    row = lax.broadcasted_iota(jnp.int32, (body, LANES), 0)
    lane = lax.broadcasted_iota(jnp.int32, (body, LANES), 1)

    def visit(d, carry):
        code = route_ref[d]

        @pl.when(code >= 0)
        def _():
            t = code // KEY_VALUE_HEADS
            g = code % KEY_VALUE_HEADS
            line = jnp.broadcast_to(reply_ref[d, body : body + 1, :], (body, LANES))
            theirs = jnp.sum(jnp.where(row == lane, line, 0.0), axis=1, keepdims=True)
            for h in range(GROUP):
                head = g * GROUP + h
                column = pl.ds(pl.multiple_of(head * HEAD_SIZE, HEAD_SIZE), HEAD_SIZE)
                place = pl.ds(pl.multiple_of((head * tiles + t) * rows, 8), rows)
                ours = run_ref[place, :]
                other = theirs[h * rows : (h + 1) * rows]
                top = jnp.maximum(ours, other)
                w_ours = jnp.exp2(ours - top)
                w_other = jnp.exp2(other - top)
                total = w_ours + w_other
                out_ref[t, :, column] = (
                    w_ours * out_ref[t, :, column]
                    + w_other * reply_ref[d, h * rows : (h + 1) * rows, :]
                ) / total
                run_ref[place, :] = top + jnp.log2(total)

        return carry

    lax.fori_loop(0, shards, visit, 0)


def on_device(queries, keys, values, selected):
    shards = lax.axis_size("ctx")
    sub_count = lax.axis_size("sub")
    ctx = lax.axis_index("ctx")
    sub = lax.axis_index("sub")
    tiles, rows, width = queries.shape
    chips = sub_count // CORES
    span = GROUP * rows + PAD
    keys = keys.reshape(keys.shape[1:])
    values = values.reshape(values.shape[1:])
    place = jnp.stack([ctx, sub, jnp.int32(sub_count)]).astype(jnp.int32)

    def swap(x):
        return lax.ppermute(x, "sub", [(s, s ^ 1) for s in range(sub_count)])

    def shift(x, step):
        return lax.ppermute(
            x, "sub", [(s, (s + step * CORES) % sub_count) for s in range(sub_count)]
        )

    far_keys = [shift(keys, step) for step in range(1, chips)]
    far_values = [shift(values, step) for step in range(1, chips)]
    near_keys, near_values = [keys, swap(keys)], [values, swap(values)]

    packed, route = pl.pallas_call(
        pack_kernel,
        out_shape=(
            jax.ShapeDtypeStruct((shards, span, LANES), jnp.float32),
            jax.ShapeDtypeStruct((shards,), jnp.int32),
        ),
        in_specs=[SMEM, SMEM, VMEM],
        out_specs=(VMEM, SMEM),
        compiler_params=PARAMS,
        name="pack",
    )(place, selected, queries)
    arrived = lax.all_to_all(packed, "ctx", split_axis=0, concat_axis=0, tiled=True)

    near_ids = jnp.stack([sub, sub ^ 1]).astype(jnp.int32)
    own_state = own_pass(True, False, place, near_ids, queries, near_keys, near_values, ())
    routed_state = routed_pass(True, False, arrived, near_keys, near_values, ())

    rest_keys, rest_values, rest_ids = [], [], []
    for step in range(1, chips):
        source = (sub - step * CORES) % sub_count
        rest_keys += [far_keys[step - 1], swap(far_keys[step - 1])]
        rest_values += [far_values[step - 1], swap(far_values[step - 1])]
        rest_ids += [source, source ^ 1]
    rest_ids = jnp.stack(rest_ids).astype(jnp.int32)
    (reply,) = routed_pass(False, True, arrived, rest_keys, rest_values, routed_state)
    answers = lax.all_to_all(reply, "ctx", split_axis=0, concat_axis=0, tiled=True)
    own_out, own_lse = own_pass(
        False, True, place, rest_ids, queries, rest_keys, rest_values, own_state
    )
    return pl.pallas_call(
        merge_kernel,
        out_shape=jax.ShapeDtypeStruct(queries.shape, jnp.float32),
        in_specs=[SMEM] + [VMEM] * 3,
        out_specs=VMEM,
        scratch_shapes=[pltpu.VMEM(own_lse.shape, jnp.float32)],
        compiler_params=PARAMS,
        name="merge",
    )(route, answers, own_out, own_lse)


def solution(mesh):
    in_specs = (
        P("ctx", "sub", None),
        P("ctx", "sub", None),
        P("ctx", "sub", None),
        P("ctx", None, None),
    )
    out_specs = P("ctx", "sub", None)
    return jax.shard_map(
        on_device, mesh=mesh, in_specs=in_specs, out_specs=out_specs, check_vma=False
    )
```

```python
import functools
import math

import jax
import jax.numpy as jnp
from jax import lax
from jax.experimental import pallas as pl
from jax.experimental.pallas import tpu as pltpu
from jax.sharding import PartitionSpec as P

QUERY_HEADS = 4
KEY_VALUE_HEADS = 2
HEAD_SIZE = 128
GROUP = QUERY_HEADS // KEY_VALUE_HEADS
CORES = 2
LANES = 128
PAD = 8

LOW_FILL = -1e30
SCALE = HEAD_SIZE ** (-0.5) * math.log2(math.e)


VMEM = pl.BlockSpec(memory_space=pltpu.VMEM)
SMEM = pl.BlockSpec(memory_space=pltpu.SMEM)
HBM = pl.BlockSpec(memory_space=pltpu.HBM)
PARAMS = pltpu.CompilerParams(vmem_limit_bytes=24 * 1024 * 1024)


def halves(x):
    high = x.astype(jnp.bfloat16)
    low = (x - high.astype(jnp.float32)).astype(jnp.bfloat16)
    return high, low


def dot_nt(a, b):
    return lax.dot_general(
        a, b, (((1,), (1,)), ((), ())), preferred_element_type=jnp.float32
    )


def dot_nn(a, b):
    return lax.dot_general(
        a, b, (((1,), (0,)), ((), ())), preferred_element_type=jnp.float32
    )


def pack_kernel(sel_ref, q_ref, packed_ref, route_ref, tag_ref, sems):
    tiles, rows, _ = q_ref.shape
    shards, span, _ = packed_ref.shape
    picks = sel_ref.shape[0]
    mine = lax.axis_index("ctx")
    for g in range(KEY_VALUE_HEADS):
        tag_ref[g] = jnp.full((PAD, LANES), g, jnp.float32)
    for d in range(shards):
        route_ref[d] = -1

    def copies(d, t, g):
        pieces = []
        for h in range(GROUP):
            column = (g * GROUP + h) * HEAD_SIZE
            pieces.append(
                pltpu.make_async_copy(
                    q_ref.at[t, :, pl.ds(column, HEAD_SIZE)],
                    packed_ref.at[d, pl.ds(h * rows, rows), :],
                    sems.at[d, h],
                )
            )
        pieces.append(
            pltpu.make_async_copy(
                tag_ref.at[g], packed_ref.at[d, pl.ds(GROUP * rows, PAD), :], sems.at[d, GROUP]
            )
        )
        return pieces

    def visit(t, carry):
        for g in range(KEY_VALUE_HEADS):
            for c in range(picks):
                d = sel_ref[c, g, t]

                @pl.when(d < mine)
                def _():
                    route_ref[d] = t * KEY_VALUE_HEADS + g
                    for piece in copies(d, t, g):
                        piece.start()

        return carry

    lax.fori_loop(0, tiles, visit, 0)

    def settle(d, carry):
        @pl.when(route_ref[d] >= 0)
        def _():
            for piece in copies(d, 0, 0):
                piece.wait()

        return carry

    lax.fori_loop(0, shards, settle, 0)


def source_of(sub, move, sub_count):
    step, swapped = move
    source = (sub - step * CORES + sub_count) % sub_count
    return source ^ 1 if swapped else source


def own_scores(offsets, sub_count, q_ref, k_refs, head_pair):
    tiles, rows, _ = q_ref.shape
    per_head = tiles * rows
    key_rows = k_refs[0].shape[0]
    sub = lax.axis_index("sub")
    tile_span = rows * sub_count
    q = jnp.concatenate(
        [
            q_ref[:, :, (head_pair * GROUP + h) * HEAD_SIZE : (head_pair * GROUP + h + 1) * HEAD_SIZE]
            .reshape(per_head, HEAD_SIZE)
            for h in range(GROUP)
        ],
        axis=0,
    )
    high, low = halves(q * SCALE)
    left = jnp.concatenate([high, low, high, low], axis=1)
    row = lax.broadcasted_iota(jnp.int32, (GROUP * per_head, key_rows), 0) % per_head
    row = row // rows * tile_span + row % rows + sub * rows
    column = lax.broadcasted_iota(jnp.int32, (GROUP * per_head, key_rows), 1)
    gap = column - row
    pieces = []
    for k_ref, offset in zip(k_refs, offsets):
        k_high, k_low = halves(k_ref[:, head_pair * HEAD_SIZE : (head_pair + 1) * HEAD_SIZE])
        right = jnp.concatenate([k_high, k_high, k_low, k_low], axis=1)
        score = dot_nt(left, right)
        pieces.append(jnp.where(gap <= -offset * key_rows, score, LOW_FILL))
    return pieces


def row_max(pieces):
    top = pieces[0]
    for piece in pieces[1:]:
        top = jnp.maximum(top, piece)
    return jnp.max(top, axis=1, keepdims=True)


def row_sum(pieces):
    total = pieces[0]
    for piece in pieces[1:]:
        total = total + piece
    return jnp.sum(total, axis=1, keepdims=True)


def own_values(weights, v_refs, head_pair):
    total = None
    for weight, v_ref in zip(weights, v_refs):
        w_high, w_low = halves(weight)
        v_high, v_low = halves(v_ref[:, head_pair * HEAD_SIZE : (head_pair + 1) * HEAD_SIZE])
        right = jnp.concatenate([v_high, v_low], axis=1)
        part = dot_nn(w_high, right) + dot_nn(w_low, right)
        total = part if total is None else total + part
    return total[:, :HEAD_SIZE] + total[:, HEAD_SIZE:]


def lines_of(lse, blocks, rows):
    height = lse.shape[0] // blocks
    wide = jnp.broadcast_to(lse, (lse.shape[0], LANES)).reshape(blocks, height, LANES)
    row = lax.broadcasted_iota(jnp.int32, wide.shape, 1)
    lane = lax.broadcasted_iota(jnp.int32, wide.shape, 2)
    return jnp.sum(jnp.where(row == lane - rows, wide, 0.0), axis=1)


def own_kernel(moves, sub_count, q_ref, *refs):
    count = len(moves)
    k_refs, v_refs, (out_ref, lse_ref) = refs[:count], refs[count : 2 * count], refs[2 * count :]
    tiles, rows, _ = q_ref.shape
    per_head = tiles * rows
    sub = lax.axis_index("sub")
    offsets = [source_of(sub, move, sub_count) for move in moves]
    for g in range(KEY_VALUE_HEADS):
        pieces = own_scores(offsets, sub_count, q_ref, k_refs, g)
        top = row_max(pieces)
        weights = [jnp.exp2(piece - top) for piece in pieces]
        total = row_sum(weights)
        out = own_values(weights, v_refs, g) / total
        lse = top + jnp.log2(total)
        lines = None
        for h in range(GROUP):
            column = (g * GROUP + h) * HEAD_SIZE
            span = slice(h * per_head, (h + 1) * per_head)
            out_ref[:, :, column : column + HEAD_SIZE] = out[span].reshape(tiles, rows, HEAD_SIZE)
            part = lines_of(lse[span], tiles, h * rows)
            lines = part if lines is None else lines + part
        lse_ref[:, g, :] = lines


def own_pass(moves, sub_count, queries, keys, values):
    tiles = queries.shape[0]
    return pl.pallas_call(
        functools.partial(own_kernel, moves, sub_count),
        out_shape=(
            jax.ShapeDtypeStruct(queries.shape, jnp.float32),
            jax.ShapeDtypeStruct((tiles, KEY_VALUE_HEADS, LANES), jnp.float32),
        ),
        in_specs=[VMEM] * (1 + 2 * len(moves)),
        out_specs=(VMEM, VMEM),
        compiler_params=PARAMS,
        name="own",
    )(queries, *keys, *values)


def routed_kernel(count, packed_ref, *refs):
    k_refs, v_refs, reply_ref = refs[:count], refs[count : 2 * count], refs[2 * count]
    shards, span, _ = packed_ref.shape
    body = span - PAD
    total_rows = shards * body
    label = jnp.broadcast_to(packed_ref[:, body : body + 1, :], (shards, body, LANES)).reshape(
        total_rows, LANES
    )
    rows = packed_ref[:, :body, :].reshape(total_rows, HEAD_SIZE)
    wide = jnp.concatenate(
        [jnp.where(label == g, rows * SCALE, 0.0) for g in range(KEY_VALUE_HEADS)], axis=1
    )
    high, low = halves(wide)
    left = jnp.concatenate([high, low, high], axis=1)
    pieces = []
    for k_ref in k_refs:
        k_high, k_low = halves(k_ref[...])
        pieces.append(dot_nt(left, jnp.concatenate([k_high, k_high, k_low], axis=1)))
    top = row_max(pieces)
    weights = [jnp.exp2(piece - top) for piece in pieces]
    total = row_sum(weights)
    result = None
    for weight, v_ref in zip(weights, v_refs):
        w_high, w_low = halves(weight)
        v_high, v_low = halves(v_ref[...])
        part = dot_nn(w_high, v_high) + dot_nn(w_low, v_high) + dot_nn(w_high, v_low)
        result = part if result is None else result + part
    acc = result[:, :HEAD_SIZE]
    for g in range(1, KEY_VALUE_HEADS):
        acc = jnp.where(label == g, result[:, g * HEAD_SIZE : (g + 1) * HEAD_SIZE], acc)
    reply_ref[:, :body, :] = (acc / total).reshape(shards, body, HEAD_SIZE)
    lines = lines_of(top + jnp.log2(total), shards, 0)
    reply_ref[:, body:, :] = jnp.broadcast_to(lines[:, None, :], (shards, PAD, LANES))


def routed_pass(packed, keys, values):
    count = len(keys)
    return pl.pallas_call(
        functools.partial(routed_kernel, count),
        out_shape=jax.ShapeDtypeStruct(packed.shape, jnp.float32),
        in_specs=[VMEM] * (1 + 2 * count),
        out_specs=VMEM,
        compiler_params=PARAMS,
        name="routed",
    )(packed, *keys, *values)


def merge_kernel(route_ref, reply_ref, own_ref, lse_ref, out_ref, run_ref):
    rows = own_ref.shape[1]
    shards, span, _ = reply_ref.shape
    body = span - PAD
    out_ref[...] = own_ref[...]
    run_ref[...] = lse_ref[...]
    row = lax.broadcasted_iota(jnp.int32, (body, LANES), 0)
    lane = lax.broadcasted_iota(jnp.int32, (body, LANES), 1)

    def stand(line):
        wide = jnp.where(row == lane, jnp.broadcast_to(line, (body, LANES)), 0.0)
        return jnp.sum(wide, axis=1, keepdims=True)

    def visit(d, carry):
        code = route_ref[d]

        @pl.when(code >= 0)
        def _():
            t = code // KEY_VALUE_HEADS
            g = code % KEY_VALUE_HEADS
            ours = run_ref[t, pl.ds(g, 1), :]
            theirs = reply_ref[d, body : body + 1, :]
            top = jnp.maximum(ours, theirs)
            w_ours = jnp.exp2(ours - top)
            w_theirs = jnp.exp2(theirs - top)
            total = w_ours + w_theirs
            run_ref[t, pl.ds(g, 1), :] = top + jnp.log2(total)
            a = stand(w_ours / total)
            b = stand(w_theirs / total)
            for h in range(GROUP):
                column = pl.ds(pl.multiple_of((g * GROUP + h) * HEAD_SIZE, HEAD_SIZE), HEAD_SIZE)
                part = slice(h * rows, (h + 1) * rows)
                out_ref[t, :, column] = (
                    a[part] * out_ref[t, :, column] + b[part] * reply_ref[d, part, :]
                )

        return carry

    lax.fori_loop(0, shards, visit, 0)


def on_device(queries, keys, values, selected):
    shards = lax.axis_size("ctx")
    sub_count = lax.axis_size("sub")
    tiles, rows, width = queries.shape
    chips = sub_count // CORES
    span = GROUP * rows + PAD
    keys = keys.reshape(keys.shape[1:])
    values = values.reshape(values.shape[1:])

    def swap(x):
        return lax.ppermute(x, "sub", [(s, s ^ 1) for s in range(sub_count)])

    def shift(x, step):
        return lax.ppermute(
            x, "sub", [(s, (s + step * CORES) % sub_count) for s in range(sub_count)]
        )

    far_keys = [shift(keys, step) for step in range(1, chips)]
    far_values = [shift(values, step) for step in range(1, chips)]
    near_keys, near_values = [keys, swap(keys)], [values, swap(values)]

    packed, route = pl.pallas_call(
        pack_kernel,
        out_shape=(
            jax.ShapeDtypeStruct((shards, span, LANES), jnp.float32),
            jax.ShapeDtypeStruct((shards,), jnp.int32),
        ),
        in_specs=[SMEM, HBM],
        out_specs=(HBM, SMEM),
        scratch_shapes=[
            pltpu.VMEM((KEY_VALUE_HEADS, PAD, LANES), jnp.float32),
            pltpu.SemaphoreType.DMA((shards, GROUP + 1)),
        ],
        compiler_params=PARAMS,
        name="pack",
    )(jnp.transpose(selected, (2, 1, 0)), pltpu.with_memory_space_constraint(queries, pltpu.HBM))
    arrived = lax.all_to_all(packed, "ctx", split_axis=0, concat_axis=0, tiled=True)

    near_moves = ((0, False), (0, True))
    far_moves = tuple((step, swapped) for step in range(1, chips) for swapped in (False, True))
    rest_keys, rest_values = [], []
    for far_key, far_value in zip(far_keys, far_values):
        rest_keys += [far_key, swap(far_key)]
        rest_values += [far_value, swap(far_value)]
    all_keys, all_values = near_keys + rest_keys, near_values + rest_values
    reply = routed_pass(arrived, all_keys, all_values)
    answers = lax.all_to_all(reply, "ctx", split_axis=0, concat_axis=0, tiled=True)
    own_out, own_lse = own_pass(near_moves + far_moves, sub_count, queries, all_keys, all_values)
    return pl.pallas_call(
        merge_kernel,
        out_shape=jax.ShapeDtypeStruct(queries.shape, jnp.float32),
        in_specs=[SMEM] + [VMEM] * 3,
        out_specs=VMEM,
        scratch_shapes=[pltpu.VMEM(own_lse.shape, jnp.float32)],
        compiler_params=PARAMS,
        name="merge",
    )(route, answers, own_out, own_lse)


def solution(mesh):
    in_specs = (
        P("ctx", "sub", None),
        P("ctx", "sub", None),
        P("ctx", "sub", None),
        P("ctx", None, None),
    )
    out_specs = P("ctx", "sub", None)
    return jax.shard_map(
        on_device, mesh=mesh, in_specs=in_specs, out_specs=out_specs, check_vma=False
    )
```

```python
import functools
import math

import jax
import jax.numpy as jnp
from jax import lax
from jax.experimental import pallas as pl
from jax.experimental.pallas import tpu as pltpu
from jax.sharding import PartitionSpec as P


QUERY_HEADS = 4
KEY_VALUE_HEADS = 2
HEAD_SIZE = 128
GROUP = QUERY_HEADS // KEY_VALUE_HEADS
CORES = 2
LANES = 128
PAD = 8

LOW_FILL = -1e30
SCALE = HEAD_SIZE ** (-0.5) * math.log2(math.e)


VMEM = pl.BlockSpec(memory_space=pltpu.VMEM)
SMEM = pl.BlockSpec(memory_space=pltpu.SMEM)
HBM = pl.BlockSpec(memory_space=pltpu.HBM)
PARAMS = pltpu.CompilerParams(vmem_limit_bytes=24 * 1024 * 1024)


def halves(x):
    high = x.astype(jnp.bfloat16)
    low = (x - high.astype(jnp.float32)).astype(jnp.bfloat16)
    return high, low


def dot_nt(a, b):
    return lax.dot_general(
        a, b, (((1,), (1,)), ((), ())), preferred_element_type=jnp.float32
    )


def dot_nn(a, b):
    return lax.dot_general(
        a, b, (((1,), (0,)), ((), ())), preferred_element_type=jnp.float32
    )


def pack_kernel(sel_hbm, q_hbm, packed_ref, route_ref, sel_ref, q_ref, sel_sem, q_sem):
    table = pltpu.make_async_copy(sel_hbm, sel_ref, sel_sem)
    table.start()
    fetch = pltpu.make_async_copy(q_hbm, q_ref, q_sem)
    fetch.start()
    tiles, rows, _ = q_ref.shape
    shards, _, _ = packed_ref.shape
    picks = sel_ref.shape[0]
    mine = lax.axis_index("ctx")
    for d in range(shards):
        route_ref[d] = -1
    table.wait()

    def visit(t, carry):
        for g in range(KEY_VALUE_HEADS):
            for c in range(picks):
                d = sel_ref[c, g, t]

                @pl.when(d < mine)
                def _():
                    route_ref[d] = t * KEY_VALUE_HEADS + g

        return carry

    lax.fori_loop(0, tiles, visit, 0)
    fetch.wait()

    def fill(d, carry):
        code = jnp.maximum(route_ref[d], 0)
        t = code // KEY_VALUE_HEADS
        g = code % KEY_VALUE_HEADS
        for h in range(GROUP):
            column = pl.multiple_of((g * GROUP + h) * HEAD_SIZE, HEAD_SIZE)
            packed_ref[d, h * rows : (h + 1) * rows, :] = q_ref[t, :, pl.ds(column, HEAD_SIZE)]
        packed_ref[d, GROUP * rows :, :] = jnp.full((PAD, LANES), g, jnp.int32).astype(jnp.float32)
        return carry

    lax.fori_loop(0, shards, fill, 0)


def source_of(sub, move, sub_count):
    step, swapped = move
    source = (sub - step * CORES + sub_count) % sub_count
    return source ^ 1 if swapped else source


def own_scores(offsets, sub_count, q_ref, k_refs, head_pair):
    tiles, rows, _ = q_ref.shape
    per_head = tiles * rows
    key_rows = k_refs[0].shape[0]
    sub = lax.axis_index("sub")
    tile_span = rows * sub_count
    q = jnp.concatenate(
        [
            q_ref[:, :, (head_pair * GROUP + h) * HEAD_SIZE : (head_pair * GROUP + h + 1) * HEAD_SIZE]
            .reshape(per_head, HEAD_SIZE)
            for h in range(GROUP)
        ],
        axis=0,
    )
    high, low = halves(q * SCALE)
    left = jnp.concatenate([high, low, high, low], axis=1)
    row = lax.broadcasted_iota(jnp.int32, (GROUP * per_head, key_rows), 0) % per_head
    row = row // rows * tile_span + row % rows + sub * rows
    column = lax.broadcasted_iota(jnp.int32, (GROUP * per_head, key_rows), 1)
    gap = column - row
    pieces = []
    for k_ref, offset in zip(k_refs, offsets):
        k_high, k_low = halves(k_ref[:, head_pair * HEAD_SIZE : (head_pair + 1) * HEAD_SIZE])
        right = jnp.concatenate([k_high, k_high, k_low, k_low], axis=1)
        score = dot_nt(left, right)
        pieces.append(jnp.where(gap <= -offset * key_rows, score, LOW_FILL))
    return pieces


def row_max(pieces):
    top = pieces[0]
    for piece in pieces[1:]:
        top = jnp.maximum(top, piece)
    return jnp.max(top, axis=1, keepdims=True)


def row_sum(pieces):
    total = pieces[0]
    for piece in pieces[1:]:
        total = total + piece
    return jnp.sum(total, axis=1, keepdims=True)


def own_values(weights, v_refs, head_pair):
    total = None
    for weight, v_ref in zip(weights, v_refs):
        w_high, w_low = halves(weight)
        v_high, v_low = halves(v_ref[:, head_pair * HEAD_SIZE : (head_pair + 1) * HEAD_SIZE])
        right = jnp.concatenate([v_high, v_low], axis=1)
        part = dot_nn(w_high, right) + dot_nn(w_low, right)
        total = part if total is None else total + part
    return total[:, :HEAD_SIZE] + total[:, HEAD_SIZE:]


def lines_of(lse, blocks, rows):
    height = lse.shape[0] // blocks
    wide = jnp.broadcast_to(lse, (lse.shape[0], LANES)).reshape(blocks, height, LANES)
    row = lax.broadcasted_iota(jnp.int32, wide.shape, 1)
    lane = lax.broadcasted_iota(jnp.int32, wide.shape, 2)
    return jnp.sum(jnp.where(row == lane - rows, wide, 0.0), axis=1)


def own_kernel(moves, sub_count, q_ref, *refs):
    count = len(moves)
    k_refs, v_refs, (base_ref, out_ref, lse_ref) = (
        refs[:count],
        refs[count : 2 * count],
        refs[2 * count :],
    )
    tiles, rows, _ = q_ref.shape
    per_head = tiles * rows
    sub = lax.axis_index("sub")
    offsets = [source_of(sub, move, sub_count) for move in moves]
    for g in range(KEY_VALUE_HEADS):
        pieces = own_scores(offsets, sub_count, q_ref, k_refs, g)
        top = row_max(pieces)
        weights = [jnp.exp2(piece - top) for piece in pieces]
        total = row_sum(weights)
        out = own_values(weights, v_refs, g) / total
        lse = top + jnp.log2(total)
        lines = None
        for h in range(GROUP):
            column = (g * GROUP + h) * HEAD_SIZE
            span = slice(h * per_head, (h + 1) * per_head)
            block = out[span].reshape(tiles, rows, HEAD_SIZE)
            base_ref[:, :, column : column + HEAD_SIZE] = block
            out_ref[:, :, column : column + HEAD_SIZE] = block
            part = lines_of(lse[span], tiles, h * rows)
            lines = part if lines is None else lines + part
        lse_ref[:, g, :] = lines


def own_pass(moves, sub_count, queries, keys, values):
    tiles = queries.shape[0]
    return pl.pallas_call(
        functools.partial(own_kernel, moves, sub_count),
        out_shape=(
            jax.ShapeDtypeStruct(queries.shape, jnp.float32),
            jax.ShapeDtypeStruct(queries.shape, jnp.float32),
            jax.ShapeDtypeStruct((tiles, KEY_VALUE_HEADS, LANES), jnp.float32),
        ),
        in_specs=[VMEM] * (1 + 2 * len(moves)),
        out_specs=(VMEM,) * 3,
        compiler_params=PARAMS,
        name="own",
    )(queries, *keys, *values)


def others(shards):
    mine = lax.axis_index("ctx")
    return [(mine + 1 + i) % shards for i in range(shards - 1)]


def pick_group(label, wide):
    picked = wide[:, :HEAD_SIZE]
    for g in range(1, KEY_VALUE_HEADS):
        picked = jnp.where(label == g, wide[:, g * HEAD_SIZE : (g + 1) * HEAD_SIZE], picked)
    return picked


def labels_of(packed_ref, slots, body):
    return jnp.concatenate(
        [jnp.broadcast_to(packed_ref[j, body : body + 1, :], (body, LANES)) for j in slots], axis=0
    )


def routed_kernel(count, packed_ref, *refs):
    k_refs, v_refs, (reply_ref, high_ref, low_ref) = (
        refs[:count],
        refs[count : 2 * count - 1],
        refs[2 * count - 1 :],
    )
    shards, span, _ = packed_ref.shape
    body = span - PAD
    slots = others(shards)
    label = labels_of(packed_ref, slots, body)
    rows = jnp.concatenate([packed_ref[j, :body, :] for j in slots], axis=0) * SCALE
    wide = jnp.concatenate(
        [jnp.where(label == g, rows, 0.0) for g in range(KEY_VALUE_HEADS)], axis=1
    )
    high, low = halves(wide)
    left = jnp.concatenate([high, low, high], axis=1)
    pieces = []
    for k_ref in k_refs:
        k_high, k_low = halves(k_ref[...])
        pieces.append(dot_nt(left, jnp.concatenate([k_high, k_high, k_low], axis=1)))
    parts = []
    for start in range(0, count, 2):
        some = pieces[start : start + 2]
        top = row_max(some)
        weights = [jnp.exp2(piece - top) for piece in some]
        total = row_sum(weights)
        result = None
        for weight, v_ref in zip(weights, v_refs[start : start + 2]):
            w_high, w_low = halves(weight)
            v_high, v_low = halves(v_ref[...])
            part = dot_nn(w_high, v_high) + dot_nn(w_low, v_high) + dot_nn(w_high, v_low)
            result = part if result is None else result + part
        parts.append((top, total, pick_group(label, result)))
    top = functools.reduce(jnp.maximum, [part[0] for part in parts])
    shrinks = [jnp.exp2(part[0] - top) for part in parts]
    total = sum(shrink * part[1] for shrink, part in zip(shrinks, parts))
    scale = 1.0 / total
    out = sum(shrink * scale * part[2] for shrink, part in zip(shrinks, parts))
    w_high, w_low = halves(weights[-1] * (shrinks[-1] * scale))
    high_ref[...] = w_high
    low_ref[...] = w_low
    lines = lines_of(top + jnp.log2(total), shards - 1, 0)
    for i, j in enumerate(slots):
        reply_ref[j, :body, :] = out[i * body : (i + 1) * body]
        reply_ref[j, body:, :] = jnp.broadcast_to(lines[i : i + 1], (PAD, LANES))


def routed_last_kernel(packed_ref, part_ref, high_ref, low_ref, v_ref, reply_ref):
    shards, span, _ = packed_ref.shape
    body = span - PAD
    slots = others(shards)
    label = labels_of(packed_ref, slots, body)
    v_high, v_low = halves(v_ref[...])
    result = (
        dot_nn(high_ref[...], v_high)
        + dot_nn(low_ref[...], v_high)
        + dot_nn(high_ref[...], v_low)
    )
    out = pick_group(label, result)
    for i, j in enumerate(slots):
        reply_ref[j, :body, :] = part_ref[j, :body, :] + out[i * body : (i + 1) * body]
        reply_ref[j, body:, :] = part_ref[j, body:, :]


def routed_pass(packed, keys, values):
    shards, span, _ = packed.shape
    count = len(keys)
    weight = jax.ShapeDtypeStruct(((shards - 1) * (span - PAD), keys[0].shape[0]), jnp.bfloat16)
    part, high, low = pl.pallas_call(
        functools.partial(routed_kernel, count),
        out_shape=(jax.ShapeDtypeStruct(packed.shape, jnp.float32), weight, weight),
        in_specs=[VMEM] * (2 * count),
        out_specs=(VMEM,) * 3,
        compiler_params=PARAMS,
        name="routed",
    )(packed, *keys, *values[:-1])
    return pl.pallas_call(
        routed_last_kernel,
        out_shape=jax.ShapeDtypeStruct(packed.shape, jnp.float32),
        in_specs=[VMEM] * 5,
        out_specs=VMEM,
        compiler_params=PARAMS,
        name="routed_last",
    )(packed, part, high, low, values[-1])


def merge_kernel(
    route_ref, reply_ref, _own, _lse, _base, own_ref, run_ref, out_ref, last_ref, sems
):
    rows = own_ref.shape[1]
    shards, span, _ = reply_ref.shape
    body = span - PAD
    width = GROUP * HEAD_SIZE

    def store(d):
        code = route_ref[d]
        t = code // KEY_VALUE_HEADS
        columns = pl.ds(pl.multiple_of(code % KEY_VALUE_HEADS * width, width), width)
        return pltpu.make_async_copy(
            own_ref.at[t, :, columns], out_ref.at[t, :, columns], sems.at[d]
        )

    def is_last(d):
        code = route_ref[d]
        return (code >= 0) & (last_ref[jnp.maximum(code, 0)] == d)

    def note(d, carry):
        code = route_ref[d]

        @pl.when(code >= 0)
        def _():
            last_ref[code] = d

        return carry

    lax.fori_loop(0, shards, note, 0)
    row = lax.broadcasted_iota(jnp.int32, (body, LANES), 0)
    lane = lax.broadcasted_iota(jnp.int32, (body, LANES), 1)

    def stand(line):
        wide = jnp.where(row == lane, jnp.broadcast_to(line, (body, LANES)), 0.0)
        return jnp.sum(wide, axis=1, keepdims=True)

    def visit(d, carry):
        code = route_ref[d]

        @pl.when(code >= 0)
        def _():
            t = code // KEY_VALUE_HEADS
            g = code % KEY_VALUE_HEADS
            ours = run_ref[t, pl.ds(g, 1), :]
            theirs = reply_ref[d, body : body + 1, :]
            top = jnp.maximum(ours, theirs)
            w_ours = jnp.exp2(ours - top)
            w_theirs = jnp.exp2(theirs - top)
            total = w_ours + w_theirs
            run_ref[t, pl.ds(g, 1), :] = top + jnp.log2(total)
            a = stand(w_ours / total)
            b = stand(w_theirs / total)
            for h in range(GROUP):
                column = pl.ds(pl.multiple_of((g * GROUP + h) * HEAD_SIZE, HEAD_SIZE), HEAD_SIZE)
                part = slice(h * rows, (h + 1) * rows)
                own_ref[t, :, column] = (
                    a[part] * own_ref[t, :, column] + b[part] * reply_ref[d, part, :]
                )

            @pl.when(last_ref[code] == d)
            def _():
                store(d).start()

        return carry

    lax.fori_loop(0, shards, visit, 0)

    def settle(d, carry):
        @pl.when(is_last(d))
        def _():
            store(d).wait()

        return carry

    lax.fori_loop(0, shards, settle, 0)


def on_device(queries, keys, values, selected):
    shards = lax.axis_size("ctx")
    sub_count = lax.axis_size("sub")
    tiles, rows, _ = queries.shape
    chips = sub_count // CORES
    span = GROUP * rows + PAD
    keys = keys.reshape(keys.shape[1:])
    values = values.reshape(values.shape[1:])

    def swap(x):
        return lax.ppermute(x, "sub", [(s, s ^ 1) for s in range(sub_count)])

    def shift(x, step):
        return lax.ppermute(
            x, "sub", [(s, (s + step * CORES) % sub_count) for s in range(sub_count)]
        )

    far_keys = [shift(keys, step) for step in range(1, chips)]
    far_values = [shift(values, step) for step in range(1, chips)]
    near_keys, near_values = [keys, swap(keys)], [values, swap(values)]

    packed, route = pl.pallas_call(
        pack_kernel,
        out_shape=(
            jax.ShapeDtypeStruct((shards, span, LANES), jnp.float32),
            jax.ShapeDtypeStruct((shards,), jnp.int32),
        ),
        in_specs=[HBM, HBM],
        out_specs=(VMEM, SMEM),
        scratch_shapes=[
            pltpu.SMEM(selected.shape[::-1], jnp.int32),
            pltpu.VMEM(queries.shape, jnp.float32),
            pltpu.SemaphoreType.DMA(()),
            pltpu.SemaphoreType.DMA(()),
        ],
        compiler_params=PARAMS,
        name="pack",
    )(
        pltpu.with_memory_space_constraint(jnp.transpose(selected, (2, 1, 0)), pltpu.HBM),
        pltpu.with_memory_space_constraint(queries, pltpu.HBM),
    )
    arrived = lax.all_to_all(packed, "ctx", split_axis=0, concat_axis=0, tiled=True)

    near_moves = ((0, False), (0, True))
    far_moves = tuple((step, swapped) for step in range(1, chips) for swapped in (False, True))
    rest_keys, rest_values = [], []
    for far_key, far_value in zip(far_keys, far_values):
        rest_keys += [far_key, swap(far_key)]
        rest_values += [far_value, swap(far_value)]
    all_keys, all_values = near_keys + rest_keys, near_values + rest_values
    reply = routed_pass(arrived, all_keys, all_values)
    answers = lax.all_to_all(reply, "ctx", split_axis=0, concat_axis=0, tiled=True)
    base, own_out, own_lse = own_pass(
        near_moves + far_moves, sub_count, queries, all_keys, all_values
    )
    return pl.pallas_call(
        merge_kernel,
        out_shape=(
            jax.ShapeDtypeStruct(own_out.shape, jnp.float32),
            jax.ShapeDtypeStruct(own_lse.shape, jnp.float32),
            jax.ShapeDtypeStruct(queries.shape, jnp.float32),
        ),
        in_specs=[SMEM, VMEM, VMEM, VMEM, HBM],
        out_specs=(VMEM, VMEM, HBM),
        input_output_aliases={2: 0, 3: 1, 4: 2},
        scratch_shapes=[
            pltpu.SMEM((tiles * KEY_VALUE_HEADS,), jnp.int32),
            pltpu.SemaphoreType.DMA((shards,)),
        ],
        compiler_params=PARAMS,
        name="merge",
    )(route, answers, own_out, own_lse, base)[2]


def solution(mesh):
    in_specs = (
        P("ctx", "sub", None),
        P("ctx", "sub", None),
        P("ctx", "sub", None),
        P("ctx", None, None),
    )
    out_specs = P("ctx", "sub", None)

    return jax.shard_map(
        on_device, mesh=mesh, in_specs=in_specs, out_specs=out_specs, check_vma=False
    )
```

```python
import functools
import math

import jax
import jax.numpy as jnp
from jax import lax
from jax.experimental import pallas as pl
from jax.experimental.pallas import tpu as pltpu
from jax.sharding import PartitionSpec as P


QUERY_HEADS = 4
KEY_VALUE_HEADS = 2
HEAD_SIZE = 128
GROUP = QUERY_HEADS // KEY_VALUE_HEADS
CORES = 2
LANES = 128
PAD = 2

LOW_FILL = -1e30
SCALE = HEAD_SIZE ** (-0.5) * math.log2(math.e)


VMEM = pl.BlockSpec(memory_space=pltpu.VMEM)
SMEM = pl.BlockSpec(memory_space=pltpu.SMEM)
HBM = pl.BlockSpec(memory_space=pltpu.HBM)
PARAMS = pltpu.CompilerParams(vmem_limit_bytes=24 * 1024 * 1024)


def halves(x):
    high = x.astype(jnp.bfloat16)
    low = (x - high.astype(jnp.float32)).astype(jnp.bfloat16)
    return high, low


def dot_nt(a, b):
    return lax.dot_general(
        a, b, (((1,), (1,)), ((), ())), preferred_element_type=jnp.float32
    )


def dot_nn(a, b):
    return lax.dot_general(
        a, b, (((1,), (0,)), ((), ())), preferred_element_type=jnp.float32
    )


def pack_kernel(sel_hbm, q_hbm, packed_ref, route_ref, sel_ref, q_ref, sel_sem, q_sem):
    table = pltpu.make_async_copy(sel_hbm, sel_ref, sel_sem)
    table.start()
    fetch = pltpu.make_async_copy(q_hbm, q_ref, q_sem)
    fetch.start()
    tiles, rows, _ = q_ref.shape
    span = GROUP * rows + PAD
    shards = packed_ref.shape[0] // span
    picks = sel_ref.shape[0]
    mine = lax.axis_index("ctx")
    for d in range(shards):
        route_ref[d] = -1
    table.wait()

    def visit(t, carry):
        for g in range(KEY_VALUE_HEADS):
            for c in range(picks):
                d = sel_ref[c, g, t]

                @pl.when(d < mine)
                def _():
                    route_ref[d] = t * KEY_VALUE_HEADS + g

        return carry

    lax.fori_loop(0, tiles, visit, 0)
    fetch.wait()

    for d in range(shards):
        code = jnp.maximum(route_ref[d], 0)
        t = code // KEY_VALUE_HEADS
        g = code % KEY_VALUE_HEADS
        for h in range(GROUP):
            column = pl.multiple_of((g * GROUP + h) * HEAD_SIZE, HEAD_SIZE)
            start = d * span + h * rows
            packed_ref[start : start + rows, :] = q_ref[t, :, pl.ds(column, HEAD_SIZE)]
        label = jnp.full((PAD, LANES), g, jnp.int32).astype(jnp.float32)
        packed_ref[d * span + GROUP * rows : (d + 1) * span, :] = label


def source_of(sub, move, sub_count):
    step, swapped = move
    source = (sub - step * CORES + sub_count) % sub_count
    return source ^ 1 if swapped else source


def own_scores(offsets, sub_count, q_ref, k_refs, head_pair):
    tiles, rows, _ = q_ref.shape
    per_head = tiles * rows
    key_rows = k_refs[0].shape[0]
    sub = lax.axis_index("sub")
    tile_span = rows * sub_count
    q = jnp.concatenate(
        [
            q_ref[:, :, (head_pair * GROUP + h) * HEAD_SIZE : (head_pair * GROUP + h + 1) * HEAD_SIZE]
            .reshape(per_head, HEAD_SIZE)
            for h in range(GROUP)
        ],
        axis=0,
    )
    high, low = halves(q * SCALE)
    left = jnp.concatenate([high, low, high, low], axis=1)
    row = lax.broadcasted_iota(jnp.int32, (GROUP * per_head, key_rows), 0) % per_head
    row = row // rows * tile_span + row % rows + sub * rows
    column = lax.broadcasted_iota(jnp.int32, (GROUP * per_head, key_rows), 1)
    gap = column - row
    pieces = []
    for k_ref, offset in zip(k_refs, offsets):
        k_high, k_low = halves(k_ref[:, head_pair * HEAD_SIZE : (head_pair + 1) * HEAD_SIZE])
        right = jnp.concatenate([k_high, k_high, k_low, k_low], axis=1)
        score = dot_nt(left, right)
        pieces.append(jnp.where(gap <= -offset * key_rows, score, LOW_FILL))
    return pieces


def row_max(pieces):
    top = pieces[0]
    for piece in pieces[1:]:
        top = jnp.maximum(top, piece)
    return jnp.max(top, axis=1, keepdims=True)


def row_sum(pieces):
    total = pieces[0]
    for piece in pieces[1:]:
        total = total + piece
    return jnp.sum(total, axis=1, keepdims=True)


def own_values(weights, v_refs, head_pair):
    total = None
    for weight, v_ref in zip(weights, v_refs):
        w_high, w_low = halves(weight)
        v_high, v_low = halves(v_ref[:, head_pair * HEAD_SIZE : (head_pair + 1) * HEAD_SIZE])
        right = jnp.concatenate([v_high, v_low], axis=1)
        part = dot_nn(w_high, right) + dot_nn(w_low, right)
        total = part if total is None else total + part
    return total[:, :HEAD_SIZE] + total[:, HEAD_SIZE:]


def lines_of(lse, blocks, rows):
    height = lse.shape[0] // blocks
    wide = jnp.broadcast_to(lse, (lse.shape[0], LANES)).reshape(blocks, height, LANES)
    row = lax.broadcasted_iota(jnp.int32, wide.shape, 1)
    lane = lax.broadcasted_iota(jnp.int32, wide.shape, 2)
    return jnp.sum(jnp.where(row == lane - rows, wide, 0.0), axis=1)


def own_kernel(moves, sub_count, q_ref, *refs):
    count = len(moves)
    k_refs, v_refs, (base_ref, out_ref, lse_ref) = (
        refs[:count],
        refs[count : 2 * count],
        refs[2 * count :],
    )
    tiles, rows, _ = q_ref.shape
    per_head = tiles * rows
    sub = lax.axis_index("sub")
    offsets = [source_of(sub, move, sub_count) for move in moves]
    for g in range(KEY_VALUE_HEADS):
        pieces = own_scores(offsets, sub_count, q_ref, k_refs, g)
        top = row_max(pieces)
        weights = [jnp.exp2(piece - top) for piece in pieces]
        total = row_sum(weights)
        out = own_values(weights, v_refs, g) / total
        lse = top + jnp.log2(total)
        lines = None
        for h in range(GROUP):
            column = (g * GROUP + h) * HEAD_SIZE
            span = slice(h * per_head, (h + 1) * per_head)
            block = out[span].reshape(tiles, rows, HEAD_SIZE)
            base_ref[:, :, column : column + HEAD_SIZE] = block
            out_ref[:, :, column : column + HEAD_SIZE] = block
            part = lines_of(lse[span], tiles, h * rows)
            lines = part if lines is None else lines + part
        lse_ref[:, g, :] = lines


def own_pass(moves, sub_count, queries, keys, values):
    tiles = queries.shape[0]
    return pl.pallas_call(
        functools.partial(own_kernel, moves, sub_count),
        out_shape=(
            jax.ShapeDtypeStruct(queries.shape, jnp.float32),
            jax.ShapeDtypeStruct(queries.shape, jnp.float32),
            jax.ShapeDtypeStruct((tiles, KEY_VALUE_HEADS, LANES), jnp.float32),
        ),
        in_specs=[VMEM] * (1 + 2 * len(moves)),
        out_specs=(VMEM,) * 3,
        compiler_params=PARAMS,
        name="own",
    )(queries, *keys, *values)


def others(shards):
    mine = lax.axis_index("ctx")
    return [(mine + 1 + i) % shards for i in range(shards - 1)]


def pick_group(label, wide):
    picked = wide[:, :HEAD_SIZE]
    for g in range(1, KEY_VALUE_HEADS):
        picked = jnp.where(label == g, wide[:, g * HEAD_SIZE : (g + 1) * HEAD_SIZE], picked)
    return picked


def labels_of(packed_ref, slots, body):
    return jnp.concatenate(
        [
            jnp.broadcast_to(packed_ref[pl.ds(j * (body + PAD) + body, 1), :], (body, LANES))
            for j in slots
        ],
        axis=0,
    )


def routed_kernel(count, shards, packed_ref, *refs):
    k_refs, v_refs, reply_ref = refs[:count], refs[count : 2 * count], refs[2 * count]
    span = packed_ref.shape[0] // shards
    body = span - PAD
    slots = others(shards)
    label = labels_of(packed_ref, slots, body)
    rows = jnp.concatenate([packed_ref[pl.ds(j * span, body), :] for j in slots], axis=0) * SCALE
    wide = jnp.concatenate(
        [jnp.where(label == g, rows, 0.0) for g in range(KEY_VALUE_HEADS)], axis=1
    )
    high, low = halves(wide)
    left = jnp.concatenate([high, low, high], axis=1)
    pieces = []
    for k_ref in k_refs:
        k_high, k_low = halves(k_ref[...])
        pieces.append(dot_nt(left, jnp.concatenate([k_high, k_high, k_low], axis=1)))
    parts = []
    for start in range(0, count, 2):
        some = pieces[start : start + 2]
        top = row_max(some)
        weights = [jnp.exp2(piece - top) for piece in some]
        total = row_sum(weights)
        result = None
        for weight, v_ref in zip(weights, v_refs[start : start + 2]):
            w_high, w_low = halves(weight)
            v_high, v_low = halves(v_ref[...])
            part = dot_nn(w_high, v_high) + dot_nn(w_low, v_high) + dot_nn(w_high, v_low)
            result = part if result is None else result + part
        parts.append((top, total, pick_group(label, result)))
    top = functools.reduce(jnp.maximum, [part[0] for part in parts])
    shrinks = [jnp.exp2(part[0] - top) for part in parts]
    total = sum(shrink * part[1] for shrink, part in zip(shrinks, parts))
    scale = 1.0 / total
    out = sum(shrink * scale * part[2] for shrink, part in zip(shrinks, parts))
    lines = lines_of(top + jnp.log2(total), shards - 1, 0)
    for i, j in enumerate(slots):
        reply_ref[pl.ds(j * span, body), :] = out[i * body : (i + 1) * body]
        reply_ref[pl.ds(j * span + body, PAD), :] = jnp.broadcast_to(lines[i : i + 1], (PAD, LANES))


def routed_pass(shards, packed, keys, values):
    count = len(keys)
    return pl.pallas_call(
        functools.partial(routed_kernel, count, shards),
        out_shape=jax.ShapeDtypeStruct(packed.shape, jnp.float32),
        in_specs=[VMEM] * (1 + 2 * count),
        out_specs=VMEM,
        compiler_params=PARAMS,
        name="routed",
    )(packed, *keys, *values)


def merge_kernel(
    route_ref, reply_ref, _own, _lse, _base, own_ref, run_ref, out_ref, last_ref, sems
):
    rows = own_ref.shape[1]
    body = GROUP * rows
    span = body + PAD
    shards = reply_ref.shape[0] // span
    width = GROUP * HEAD_SIZE

    def store(d):
        code = route_ref[d]
        t = code // KEY_VALUE_HEADS
        columns = pl.ds(pl.multiple_of(code % KEY_VALUE_HEADS * width, width), width)
        return pltpu.make_async_copy(
            own_ref.at[t, :, columns], out_ref.at[t, :, columns], sems.at[d]
        )

    def is_last(d):
        code = route_ref[d]
        return (code >= 0) & (last_ref[jnp.maximum(code, 0)] == d)

    def note(d, carry):
        code = route_ref[d]

        @pl.when(code >= 0)
        def _():
            last_ref[code] = d

        return carry

    lax.fori_loop(0, shards, note, 0)
    row = lax.broadcasted_iota(jnp.int32, (body, LANES), 0)
    lane = lax.broadcasted_iota(jnp.int32, (body, LANES), 1)

    def stand(line):
        wide = jnp.where(row == lane, jnp.broadcast_to(line, (body, LANES)), 0.0)
        return jnp.sum(wide, axis=1, keepdims=True)

    def visit(d, carry):
        code = route_ref[d]

        @pl.when(code >= 0)
        def _():
            t = code // KEY_VALUE_HEADS
            g = code % KEY_VALUE_HEADS
            ours = run_ref[t, pl.ds(g, 1), :]
            theirs = reply_ref[pl.ds(d * span + body, 1), :]
            top = jnp.maximum(ours, theirs)
            w_ours = jnp.exp2(ours - top)
            w_theirs = jnp.exp2(theirs - top)
            total = w_ours + w_theirs
            run_ref[t, pl.ds(g, 1), :] = top + jnp.log2(total)
            a = stand(w_ours / total)
            b = stand(w_theirs / total)
            for h in range(GROUP):
                column = pl.ds(pl.multiple_of((g * GROUP + h) * HEAD_SIZE, HEAD_SIZE), HEAD_SIZE)
                part = slice(h * rows, (h + 1) * rows)
                own_ref[t, :, column] = (
                    a[part] * own_ref[t, :, column]
                    + b[part] * reply_ref[pl.ds(d * span + h * rows, rows), :]
                )

            @pl.when(last_ref[code] == d)
            def _():
                store(d).start()

        return carry

    lax.fori_loop(0, shards, visit, 0)

    def settle(d, carry):
        @pl.when(is_last(d))
        def _():
            store(d).wait()

        return carry

    lax.fori_loop(0, shards, settle, 0)


def on_device(queries, keys, values, selected):
    shards = lax.axis_size("ctx")
    sub_count = lax.axis_size("sub")
    tiles, rows, _ = queries.shape
    chips = sub_count // CORES
    span = GROUP * rows + PAD
    keys = keys.reshape(keys.shape[1:])
    values = values.reshape(values.shape[1:])

    def exchange(x):
        parted = x.reshape(shards, span // PAD, PAD, LANES)
        moved = lax.all_to_all(parted, "ctx", split_axis=0, concat_axis=0, tiled=True)
        return moved.reshape(x.shape)

    def swap(x):
        return lax.ppermute(x, "sub", [(s, s ^ 1) for s in range(sub_count)])

    def shift(x, step):
        return lax.ppermute(
            x, "sub", [(s, (s + step * CORES) % sub_count) for s in range(sub_count)]
        )

    far_keys = [shift(keys, step) for step in range(1, chips)]
    far_values = [shift(values, step) for step in range(1, chips)]
    near_keys, near_values = [keys, swap(keys)], [values, swap(values)]

    packed, route = pl.pallas_call(
        pack_kernel,
        out_shape=(
            jax.ShapeDtypeStruct((shards * span, LANES), jnp.float32),
            jax.ShapeDtypeStruct((shards,), jnp.int32),
        ),
        in_specs=[HBM, HBM],
        out_specs=(VMEM, SMEM),
        scratch_shapes=[
            pltpu.SMEM(selected.shape[::-1], jnp.int32),
            pltpu.VMEM(queries.shape, jnp.float32),
            pltpu.SemaphoreType.DMA(()),
            pltpu.SemaphoreType.DMA(()),
        ],
        compiler_params=PARAMS,
        name="pack",
    )(
        pltpu.with_memory_space_constraint(jnp.transpose(selected, (2, 1, 0)), pltpu.HBM),
        pltpu.with_memory_space_constraint(queries, pltpu.HBM),
    )
    arrived = exchange(packed)

    near_moves = ((0, False), (0, True))
    far_moves = tuple((step, swapped) for step in range(1, chips) for swapped in (False, True))
    rest_keys, rest_values = [], []
    for far_key, far_value in zip(far_keys, far_values):
        rest_keys += [far_key, swap(far_key)]
        rest_values += [far_value, swap(far_value)]
    all_keys, all_values = near_keys + rest_keys, near_values + rest_values
    reply = routed_pass(shards, arrived, all_keys, all_values)
    answers = exchange(reply)
    base, own_out, own_lse = own_pass(
        near_moves + far_moves, sub_count, queries, all_keys, all_values
    )
    return pl.pallas_call(
        merge_kernel,
        out_shape=(
            jax.ShapeDtypeStruct(own_out.shape, jnp.float32),
            jax.ShapeDtypeStruct(own_lse.shape, jnp.float32),
            jax.ShapeDtypeStruct(queries.shape, jnp.float32),
        ),
        in_specs=[SMEM, VMEM, VMEM, VMEM, HBM],
        out_specs=(VMEM, VMEM, HBM),
        input_output_aliases={2: 0, 3: 1, 4: 2},
        scratch_shapes=[
            pltpu.SMEM((tiles * KEY_VALUE_HEADS,), jnp.int32),
            pltpu.SemaphoreType.DMA((shards,)),
        ],
        compiler_params=PARAMS,
        name="merge",
    )(route, answers, own_out, own_lse, base)[2]


def solution(mesh):
    in_specs = (
        P("ctx", "sub", None),
        P("ctx", "sub", None),
        P("ctx", "sub", None),
        P("ctx", None, None),
    )
    out_specs = P("ctx", "sub", None)

    return jax.shard_map(
        on_device, mesh=mesh, in_specs=in_specs, out_specs=out_specs, check_vma=False
    )
```

```python
import functools
import math

import jax
import jax.numpy as jnp
from jax import lax
from jax.experimental import pallas as pl
from jax.experimental.pallas import tpu as pltpu
from jax.sharding import PartitionSpec as P


QUERY_HEADS = 4
KEY_VALUE_HEADS = 2
HEAD_SIZE = 128
GROUP = QUERY_HEADS // KEY_VALUE_HEADS
CORES = 2
LANES = 128
PAD = 2

LOW_FILL = -1e30
SCALE = HEAD_SIZE ** (-0.5) * math.log2(math.e)


VMEM = pl.BlockSpec(memory_space=pltpu.VMEM)
SMEM = pl.BlockSpec(memory_space=pltpu.SMEM)
HBM = pl.BlockSpec(memory_space=pltpu.HBM)
PARAMS = pltpu.CompilerParams(vmem_limit_bytes=24 * 1024 * 1024)


def halves(x):
    high = x.astype(jnp.bfloat16)
    low = (x - high.astype(jnp.float32)).astype(jnp.bfloat16)
    return high, low


def dot_nt(a, b):
    return lax.dot_general(
        a, b, (((1,), (1,)), ((), ())), preferred_element_type=jnp.float32
    )


def dot_nn(a, b):
    return lax.dot_general(
        a, b, (((1,), (0,)), ((), ())), preferred_element_type=jnp.float32
    )


def pack_kernel(
    sel_hbm, q_hbm, packed_ref, route_ref, sel_ref, found_ref, q_ref, sel_sem, q_sem
):
    table = pltpu.make_async_copy(sel_hbm, sel_ref, sel_sem)
    table.start()
    tiles, rows, _ = q_ref.shape
    fetches = [
        pltpu.make_async_copy(q_hbm.at[pl.ds(t, 2)], q_ref.at[pl.ds(t, 2)], q_sem.at[t // 2])
        for t in range(0, tiles, 2)
    ]
    for fetch in fetches:
        fetch.start()
    span = GROUP * rows + PAD
    shards = packed_ref.shape[0] // span
    picks = sel_ref.shape[0]
    mine = lax.axis_index("ctx")
    for d in range(shards):
        found_ref[d] = -1
    table.wait()
    for t in range(tiles):
        for g in range(KEY_VALUE_HEADS):
            for c in range(picks):
                d = sel_ref[c, g, t]
                found_ref[jnp.where(d < mine, d, shards)] = t * KEY_VALUE_HEADS + g
    for fetch in fetches:
        fetch.wait()

    for d in range(shards):
        route_ref[d] = found_ref[d]
        code = jnp.maximum(found_ref[d], 0)
        t = code // KEY_VALUE_HEADS
        g = code % KEY_VALUE_HEADS
        for h in range(GROUP):
            column = pl.multiple_of((g * GROUP + h) * HEAD_SIZE, HEAD_SIZE)
            start = d * span + h * rows
            packed_ref[start : start + rows, :] = q_ref[t, :, pl.ds(column, HEAD_SIZE)]
        label = jnp.full((PAD, LANES), g, jnp.int32).astype(jnp.float32)
        packed_ref[d * span + GROUP * rows : (d + 1) * span, :] = label


def source_of(sub, move, sub_count):
    step, swapped = move
    source = (sub - step * CORES + sub_count) % sub_count
    return source ^ 1 if swapped else source


def own_scores(offsets, sub_count, q_ref, k_refs, head_pair):
    tiles, rows, _ = q_ref.shape
    per_head = tiles * rows
    key_rows = k_refs[0].shape[0]
    sub = lax.axis_index("sub")
    tile_span = rows * sub_count
    q = jnp.concatenate(
        [
            q_ref[:, :, (head_pair * GROUP + h) * HEAD_SIZE : (head_pair * GROUP + h + 1) * HEAD_SIZE]
            .reshape(per_head, HEAD_SIZE)
            for h in range(GROUP)
        ],
        axis=0,
    )
    high, low = halves(q * SCALE)
    left = jnp.concatenate([high, low, high, low], axis=1)
    row = lax.broadcasted_iota(jnp.int32, (GROUP * per_head, key_rows), 0) % per_head
    row = row // rows * tile_span + row % rows + sub * rows
    column = lax.broadcasted_iota(jnp.int32, (GROUP * per_head, key_rows), 1)
    gap = column - row
    pieces = []
    for k_ref, offset in zip(k_refs, offsets):
        k_high, k_low = halves(k_ref[:, head_pair * HEAD_SIZE : (head_pair + 1) * HEAD_SIZE])
        right = jnp.concatenate([k_high, k_high, k_low, k_low], axis=1)
        score = dot_nt(left, right)
        pieces.append(jnp.where(gap <= -offset * key_rows, score, LOW_FILL))
    return pieces


def row_max(pieces):
    top = pieces[0]
    for piece in pieces[1:]:
        top = jnp.maximum(top, piece)
    return jnp.max(top, axis=1, keepdims=True)


def row_sum(pieces):
    total = pieces[0]
    for piece in pieces[1:]:
        total = total + piece
    return jnp.sum(total, axis=1, keepdims=True)


def own_values(weights, v_refs, head_pair):
    total = None
    for weight, v_ref in zip(weights, v_refs):
        w_high, w_low = halves(weight)
        v_high, v_low = halves(v_ref[:, head_pair * HEAD_SIZE : (head_pair + 1) * HEAD_SIZE])
        right = jnp.concatenate([v_high, v_low], axis=1)
        part = dot_nn(w_high, right) + dot_nn(w_low, right)
        total = part if total is None else total + part
    return total[:, :HEAD_SIZE] + total[:, HEAD_SIZE:]


def lines_of(lse, blocks, rows):
    height = lse.shape[0] // blocks
    wide = jnp.broadcast_to(lse, (lse.shape[0], LANES)).reshape(blocks, height, LANES)
    row = lax.broadcasted_iota(jnp.int32, wide.shape, 1)
    lane = lax.broadcasted_iota(jnp.int32, wide.shape, 2)
    return jnp.sum(jnp.where(row == lane - rows, wide, 0.0), axis=1)


def own_kernel(moves, sub_count, route_ref, q_ref, *refs):
    count = len(moves)
    k_refs, v_refs, rest = refs[:count], refs[count : 2 * count], refs[2 * count :]
    base_ref, out_ref, ours_ref, same_ref, flag_ref, lse_ref, code_ref, seen_ref = rest
    tiles, rows, _ = q_ref.shape
    per_head = tiles * rows
    sub = lax.axis_index("sub")
    offsets = [source_of(sub, move, sub_count) for move in moves]
    for g in range(KEY_VALUE_HEADS):
        pieces = own_scores(offsets, sub_count, q_ref, k_refs, g)
        top = row_max(pieces)
        weights = [jnp.exp2(piece - top) for piece in pieces]
        total = row_sum(weights)
        out = own_values(weights, v_refs, g) / total
        lse = top + jnp.log2(total)
        lines = None
        for h in range(GROUP):
            column = (g * GROUP + h) * HEAD_SIZE
            span = slice(h * per_head, (h + 1) * per_head)
            block = out[span].reshape(tiles, rows, HEAD_SIZE)
            base_ref[:, :, column : column + HEAD_SIZE] = block
            out_ref[:, :, column : column + HEAD_SIZE] = block
            part = lines_of(lse[span], tiles, h * rows)
            lines = part if lines is None else lines + part
        lse_ref[:, g, :] = lines


    shards = ours_ref.shape[0]
    blank = seen_ref.shape[1] - 1
    spots = []
    for d in range(shards):
        code = route_ref[d]
        code_ref[d : d + 1, :] = jnp.full((1, LANES), code, jnp.int32)
        t = jnp.maximum(code, 0) // KEY_VALUE_HEADS
        g = jnp.maximum(code, 0) % KEY_VALUE_HEADS
        ours_ref[d : d + 1, :] = lse_ref[t, pl.ds(g, 1), :]
        spots.append(jnp.where(code >= 0, code, blank))
    for d in range(shards):
        seen_ref[0, spots[shards - 1 - d]] = shards - 1 - d
        seen_ref[1, spots[d]] = d
    for d in range(shards):
        first = (seen_ref[0, spots[d]] == d).astype(jnp.int32)
        last = (seen_ref[1, spots[d]] == d).astype(jnp.int32)
        flag_ref[d] = jnp.where(route_ref[d] >= 0, route_ref[d] * 4 + first * 2 + last, -1)
    codes = code_ref[...]
    for d in range(shards):
        match = (codes == code_ref[d : d + 1, :]) & (codes >= 0)
        same_ref[d] = jnp.where(match, 1.0, 0.0)


def own_pass(moves, sub_count, shards, route, queries, keys, values):
    tiles = queries.shape[0]
    return pl.pallas_call(
        functools.partial(own_kernel, moves, sub_count),
        out_shape=(
            jax.ShapeDtypeStruct(queries.shape, jnp.float32),
            jax.ShapeDtypeStruct(queries.shape, jnp.float32),
            jax.ShapeDtypeStruct((shards, LANES), jnp.float32),
            jax.ShapeDtypeStruct((shards, shards, LANES), jnp.float32),
            jax.ShapeDtypeStruct((shards,), jnp.int32),
        ),
        in_specs=[SMEM] + [VMEM] * (1 + 2 * len(moves)),
        out_specs=(VMEM,) * 4 + (SMEM,),
        scratch_shapes=[
            pltpu.VMEM((tiles, KEY_VALUE_HEADS, LANES), jnp.float32),
            pltpu.VMEM((shards, LANES), jnp.int32),
            pltpu.SMEM((2, tiles * KEY_VALUE_HEADS + 1), jnp.int32),
        ],
        compiler_params=PARAMS,
        name="own",
    )(route, queries, *keys, *values)


def others(shards):
    mine = lax.axis_index("ctx")
    return [(mine + 1 + i) % shards for i in range(shards - 1)]


def pick_group(label, wide):
    picked = wide[:, :HEAD_SIZE]
    for g in range(1, KEY_VALUE_HEADS):
        picked = jnp.where(label == g, wide[:, g * HEAD_SIZE : (g + 1) * HEAD_SIZE], picked)
    return picked


def labels_of(packed_ref, slots, body):
    return jnp.concatenate(
        [
            jnp.broadcast_to(packed_ref[pl.ds(j * (body + PAD) + body, 1), :], (body, LANES))
            for j in slots
        ],
        axis=0,
    )


def routed_kernel(count, shards, packed_ref, *refs):
    k_refs, v_refs, reply_ref = refs[:count], refs[count : 2 * count], refs[2 * count]
    span = packed_ref.shape[0] // shards
    body = span - PAD
    slots = others(shards)
    label = labels_of(packed_ref, slots, body)
    rows = jnp.concatenate([packed_ref[pl.ds(j * span, body), :] for j in slots], axis=0) * SCALE
    wide = jnp.concatenate(
        [jnp.where(label == g, rows, 0.0) for g in range(KEY_VALUE_HEADS)], axis=1
    )
    high, low = halves(wide)
    left = jnp.concatenate([high, low, high], axis=1)
    pieces = []
    for k_ref in k_refs:
        k_high, k_low = halves(k_ref[...])
        pieces.append(dot_nt(left, jnp.concatenate([k_high, k_high, k_low], axis=1)))
    parts = []
    for start in range(0, count, 2):
        some = pieces[start : start + 2]
        top = row_max(some)
        weights = [jnp.exp2(piece - top) for piece in some]
        total = row_sum(weights)
        result = None
        for weight, v_ref in zip(weights, v_refs[start : start + 2]):
            w_high, w_low = halves(weight)
            v_high, v_low = halves(v_ref[...])
            part = dot_nn(w_high, v_high) + dot_nn(w_low, v_high) + dot_nn(w_high, v_low)
            result = part if result is None else result + part
        parts.append((top, total, pick_group(label, result)))
    top = functools.reduce(jnp.maximum, [part[0] for part in parts])
    shrinks = [jnp.exp2(part[0] - top) for part in parts]
    total = sum(shrink * part[1] for shrink, part in zip(shrinks, parts))
    scale = 1.0 / total
    out = sum(shrink * scale * part[2] for shrink, part in zip(shrinks, parts))
    lines = lines_of(top + jnp.log2(total), shards - 1, 0)
    for i, j in enumerate(slots):
        reply_ref[pl.ds(j * span, body), :] = out[i * body : (i + 1) * body]
        reply_ref[pl.ds(j * span + body, PAD), :] = jnp.broadcast_to(lines[i : i + 1], (PAD, LANES))


def routed_pass(shards, packed, keys, values):
    count = len(keys)
    return pl.pallas_call(
        functools.partial(routed_kernel, count, shards),
        out_shape=jax.ShapeDtypeStruct(packed.shape, jnp.float32),
        in_specs=[VMEM] * (1 + 2 * count),
        out_specs=VMEM,
        compiler_params=PARAMS,
        name="routed",
    )(packed, *keys, *values)


def merge_kernel(
    flag_vmem, reply_ref, ours_ref, same_ref, _own, _base, own_ref, out_ref, flag_ref, flag_sem, sems
):
    table = pltpu.make_async_copy(flag_vmem, flag_ref, flag_sem)
    table.start()
    rows = own_ref.shape[1]
    body = GROUP * rows
    span = body + PAD
    shards = ours_ref.shape[0]
    width = GROUP * HEAD_SIZE
    ours = ours_ref[...]
    lines = [reply_ref[d * span + body : d * span + body + 1, :] for d in range(shards)]
    match = [same_ref[d] > 0.5 for d in range(shards)]
    top = ours
    for d in range(shards):
        top = jnp.maximum(top, jnp.where(match[d], lines[d], LOW_FILL))
    w_ours = jnp.exp2(ours - top)
    total = w_ours
    for d in range(shards):
        total = total + jnp.where(match[d], jnp.exp2(lines[d] - top), 0.0)
    scale = 1.0 / total
    w_ours = w_ours * scale
    w_theirs = jnp.exp2(jnp.concatenate(lines, axis=0) - top) * scale
    row = lax.broadcasted_iota(jnp.int32, (body, LANES), 0)
    lane = lax.broadcasted_iota(jnp.int32, (body, LANES), 1)

    def stand(line):
        wide = jnp.where(row == lane, jnp.broadcast_to(line, (body, LANES)), 0.0)
        return jnp.sum(wide, axis=1, keepdims=True)

    pairs = [(stand(w_ours[d : d + 1]), stand(w_theirs[d : d + 1])) for d in range(shards)]

    table.wait()
    flags = [flag_ref[d] for d in range(shards)]

    def store(d):
        code = flags[d] // 4
        t = code // KEY_VALUE_HEADS
        columns = pl.ds(pl.multiple_of(code % KEY_VALUE_HEADS * width, width), width)
        return pltpu.make_async_copy(
            own_ref.at[t, :, columns], out_ref.at[t, :, columns], sems.at[d]
        )

    for d in range(shards):

        @pl.when(flags[d] >= 0)
        def _():
            code = flags[d] // 4
            t = code // KEY_VALUE_HEADS
            g = code % KEY_VALUE_HEADS
            a = jnp.where(flags[d] // 2 % 2 == 1, pairs[d][0], 1.0)
            b = pairs[d][1]
            for h in range(GROUP):
                column = pl.ds(pl.multiple_of((g * GROUP + h) * HEAD_SIZE, HEAD_SIZE), HEAD_SIZE)
                part = slice(h * rows, (h + 1) * rows)
                start = d * span + h * rows
                own_ref[t, :, column] = (
                    a[part] * own_ref[t, :, column] + b[part] * reply_ref[start : start + rows, :]
                )

            @pl.when(flags[d] % 2 == 1)
            def _():
                store(d).start()

    for d in range(shards):

        @pl.when((flags[d] >= 0) & (flags[d] % 2 == 1))
        def _():
            store(d).wait()


def on_device(queries, keys, values, selected):
    shards = lax.axis_size("ctx")
    sub_count = lax.axis_size("sub")
    tiles, rows, _ = queries.shape
    chips = sub_count // CORES
    span = GROUP * rows + PAD
    keys = keys.reshape(keys.shape[1:])
    values = values.reshape(values.shape[1:])

    def exchange(x):
        parted = x.reshape(shards, span // PAD, PAD, LANES)
        moved = lax.all_to_all(parted, "ctx", split_axis=0, concat_axis=0, tiled=True)
        return moved.reshape(x.shape)

    def swap(x):
        return lax.ppermute(x, "sub", [(s, s ^ 1) for s in range(sub_count)])

    def shift(x, step):
        return lax.ppermute(
            x, "sub", [(s, (s + step * CORES) % sub_count) for s in range(sub_count)]
        )

    far_keys = [shift(keys, step) for step in range(1, chips)]
    far_values = [shift(values, step) for step in range(1, chips)]
    near_keys, near_values = [keys, swap(keys)], [values, swap(values)]

    packed, route = pl.pallas_call(
        pack_kernel,
        out_shape=(
            jax.ShapeDtypeStruct((shards * span, LANES), jnp.float32),
            jax.ShapeDtypeStruct((shards,), jnp.int32),
        ),
        in_specs=[HBM, HBM],
        out_specs=(VMEM, SMEM),
        scratch_shapes=[
            pltpu.SMEM(selected.shape[::-1], jnp.int32),
            pltpu.SMEM((shards + 1,), jnp.int32),
            pltpu.VMEM(queries.shape, jnp.float32),
            pltpu.SemaphoreType.DMA(()),
            pltpu.SemaphoreType.DMA((tiles // 2,)),
        ],
        compiler_params=PARAMS,
        name="pack",
    )(
        pltpu.with_memory_space_constraint(jnp.transpose(selected, (2, 1, 0)), pltpu.HBM),
        pltpu.with_memory_space_constraint(queries, pltpu.HBM),
    )
    arrived = exchange(packed)

    near_moves = ((0, False), (0, True))
    far_moves = tuple((step, swapped) for step in range(1, chips) for swapped in (False, True))
    rest_keys, rest_values = [], []
    for far_key, far_value in zip(far_keys, far_values):
        rest_keys += [far_key, swap(far_key)]
        rest_values += [far_value, swap(far_value)]
    all_keys, all_values = near_keys + rest_keys, near_values + rest_values
    reply = routed_pass(shards, arrived, all_keys, all_values)
    answers = exchange(reply)
    base, own_out, ours, same, flags = own_pass(
        near_moves + far_moves, sub_count, shards, route, queries, all_keys, all_values
    )
    return pl.pallas_call(
        merge_kernel,
        out_shape=(
            jax.ShapeDtypeStruct(own_out.shape, jnp.float32),
            jax.ShapeDtypeStruct(queries.shape, jnp.float32),
        ),
        in_specs=[VMEM, VMEM, VMEM, VMEM, VMEM, HBM],
        out_specs=(VMEM, HBM),
        input_output_aliases={4: 0, 5: 1},
        scratch_shapes=[
            pltpu.SMEM((shards,), jnp.int32),
            pltpu.SemaphoreType.DMA(()),
            pltpu.SemaphoreType.DMA((shards,)),
        ],
        compiler_params=PARAMS,
        name="merge",
    )(flags, answers, ours, same, own_out, base)[1]


def solution(mesh):
    in_specs = (
        P("ctx", "sub", None),
        P("ctx", "sub", None),
        P("ctx", "sub", None),
        P("ctx", None, None),
    )
    out_specs = P("ctx", "sub", None)

    return jax.shard_map(
        on_device, mesh=mesh, in_specs=in_specs, out_specs=out_specs, check_vma=False
    )
```

```python
import functools
import math

import jax
import jax.numpy as jnp
import numpy as np
from jax import lax
from jax.experimental import pallas as pl
from jax.experimental.pallas import tpu as pltpu
from jax.sharding import PartitionSpec as P


QUERY_HEADS = 4
KEY_VALUE_HEADS = 2
HEAD_SIZE = 128
GROUP = QUERY_HEADS // KEY_VALUE_HEADS
CORES = 2
LANES = 128
PAD = 2
SEND_LEAD = 0.5
REPLY_LEAD = 0.5

LOW_FILL = -1e30
SCALE = HEAD_SIZE ** (-0.5) * math.log2(math.e)


VMEM = pl.BlockSpec(memory_space=pltpu.VMEM)
SMEM = pl.BlockSpec(memory_space=pltpu.SMEM)
HBM = pl.BlockSpec(memory_space=pltpu.HBM)
PARAMS = pltpu.CompilerParams(vmem_limit_bytes=24 * 1024 * 1024)


def spot_of(d, lead, shards):
    return (d + shards - int(lead * shards)) % shards


def halves(x):
    high = x.astype(jnp.bfloat16)
    low = (x - high.astype(jnp.float32)).astype(jnp.bfloat16)
    return high, low


def dot_nt(a, b):
    return lax.dot_general(
        a, b, (((1,), (1,)), ((), ())), preferred_element_type=jnp.float32
    )


def dot_nn(a, b):
    return lax.dot_general(
        a, b, (((1,), (0,)), ((), ())), preferred_element_type=jnp.float32
    )


def pack_kernel(
    sel_hbm, q_hbm, packed_ref, route_ref, sel_ref, found_ref, q_ref, sel_sem, q_sem
):
    table = pltpu.make_async_copy(sel_hbm, sel_ref, sel_sem)
    table.start()
    tiles, rows, _ = q_ref.shape
    fetches = [
        pltpu.make_async_copy(q_hbm.at[pl.ds(t, 2)], q_ref.at[pl.ds(t, 2)], q_sem.at[t // 2])
        for t in range(0, tiles, 2)
    ]
    for fetch in fetches:
        fetch.start()
    span = GROUP * rows + PAD
    shards = packed_ref.shape[0] // span
    picks = sel_ref.shape[0]
    mine = lax.axis_index("ctx")
    for d in range(shards):
        found_ref[d] = -1
    table.wait()
    for t in range(tiles):
        for g in range(KEY_VALUE_HEADS):
            for c in range(picks):
                d = sel_ref[c, g, t]
                found_ref[jnp.where(d < mine, d, shards)] = t * KEY_VALUE_HEADS + g
    for fetch in fetches:
        fetch.wait()

    for d in range(shards):
        route_ref[d] = found_ref[d]
        code = jnp.maximum(found_ref[d], 0)
        t = code // KEY_VALUE_HEADS
        g = code % KEY_VALUE_HEADS
        for h in range(GROUP):
            column = pl.multiple_of((g * GROUP + h) * HEAD_SIZE, HEAD_SIZE)
            start = spot_of(d, SEND_LEAD, shards) * span + h * rows
            packed_ref[start : start + rows, :] = q_ref[t, :, pl.ds(column, HEAD_SIZE)]
        label = jnp.full((PAD, LANES), g, jnp.int32).astype(jnp.float32)
        end = (spot_of(d, SEND_LEAD, shards) + 1) * span
        packed_ref[end - PAD : end, :] = label


def source_of(sub, move, sub_count):
    step, swapped = move
    source = (sub - step * CORES + sub_count) % sub_count
    return source ^ 1 if swapped else source


def own_scores(offsets, sub_count, q_ref, k_refs, head_pair):
    tiles, rows, _ = q_ref.shape
    per_head = tiles * rows
    key_rows = k_refs[0].shape[0]
    sub = lax.axis_index("sub")
    tile_span = rows * sub_count
    q = jnp.concatenate(
        [
            q_ref[:, :, (head_pair * GROUP + h) * HEAD_SIZE : (head_pair * GROUP + h + 1) * HEAD_SIZE]
            .reshape(per_head, HEAD_SIZE)
            for h in range(GROUP)
        ],
        axis=0,
    )
    high, low = halves(q * SCALE)
    left = jnp.concatenate([high, low, high, low], axis=1)
    row = lax.broadcasted_iota(jnp.int32, (GROUP * per_head, key_rows), 0) % per_head
    row = row // rows * tile_span + row % rows + sub * rows
    column = lax.broadcasted_iota(jnp.int32, (GROUP * per_head, key_rows), 1)
    gap = column - row
    pieces = []
    for k_ref, offset in zip(k_refs, offsets):
        k_high, k_low = halves(k_ref[:, head_pair * HEAD_SIZE : (head_pair + 1) * HEAD_SIZE])
        right = jnp.concatenate([k_high, k_high, k_low, k_low], axis=1)
        score = dot_nt(left, right)
        pieces.append(jnp.where(gap <= -offset * key_rows, score, LOW_FILL))
    return pieces


def row_max(pieces):
    top = pieces[0]
    for piece in pieces[1:]:
        top = jnp.maximum(top, piece)
    return jnp.max(top, axis=1, keepdims=True)


def row_sum(pieces):
    total = pieces[0]
    for piece in pieces[1:]:
        total = total + piece
    return jnp.sum(total, axis=1, keepdims=True)


def own_values(weights, v_refs, head_pair):
    total = None
    for weight, v_ref in zip(weights, v_refs):
        w_high, w_low = halves(weight)
        v_high, v_low = halves(v_ref[:, head_pair * HEAD_SIZE : (head_pair + 1) * HEAD_SIZE])
        right = jnp.concatenate([v_high, v_low], axis=1)
        part = dot_nn(w_high, right) + dot_nn(w_low, right)
        total = part if total is None else total + part
    return total[:, :HEAD_SIZE] + total[:, HEAD_SIZE:]


def lines_of(lse, blocks, rows):
    height = lse.shape[0] // blocks
    wide = jnp.broadcast_to(lse, (lse.shape[0], LANES)).reshape(blocks, height, LANES)
    row = lax.broadcasted_iota(jnp.int32, wide.shape, 1)
    lane = lax.broadcasted_iota(jnp.int32, wide.shape, 2)
    return jnp.sum(jnp.where(row == lane - rows, wide, 0.0), axis=1)


def own_kernel(moves, sub_count, route_ref, q_ref, *refs):
    count = len(moves)
    k_refs, v_refs, rest = refs[:count], refs[count : 2 * count], refs[2 * count :]
    base_ref, out_ref, ours_ref, same_ref, flag_ref, lse_ref, code_ref, seen_ref = rest
    tiles, rows, _ = q_ref.shape
    per_head = tiles * rows
    sub = lax.axis_index("sub")
    offsets = [source_of(sub, move, sub_count) for move in moves]
    for g in range(KEY_VALUE_HEADS):
        pieces = own_scores(offsets, sub_count, q_ref, k_refs, g)
        top = row_max(pieces)
        weights = [jnp.exp2(piece - top) for piece in pieces]
        total = row_sum(weights)
        out = own_values(weights, v_refs, g) / total
        lse = top + jnp.log2(total)
        lines = None
        for h in range(GROUP):
            column = (g * GROUP + h) * HEAD_SIZE
            span = slice(h * per_head, (h + 1) * per_head)
            block = out[span].reshape(tiles, rows, HEAD_SIZE)
            base_ref[:, :, column : column + HEAD_SIZE] = block
            out_ref[:, :, column : column + HEAD_SIZE] = block
            part = lines_of(lse[span], tiles, h * rows)
            lines = part if lines is None else lines + part
        lse_ref[:, g, :] = lines


    shards = ours_ref.shape[0]
    blank = seen_ref.shape[1] - 1
    spots = []
    for d in range(shards):
        code = route_ref[d]
        code_ref[d : d + 1, :] = jnp.full((1, LANES), code, jnp.int32)
        t = jnp.maximum(code, 0) // KEY_VALUE_HEADS
        g = jnp.maximum(code, 0) % KEY_VALUE_HEADS
        ours_ref[d : d + 1, :] = lse_ref[t, pl.ds(g, 1), :]
        spots.append(jnp.where(code >= 0, code, blank))
    for d in range(shards):
        seen_ref[0, spots[shards - 1 - d]] = shards - 1 - d
        seen_ref[1, spots[d]] = d
    for d in range(shards):
        first = (seen_ref[0, spots[d]] == d).astype(jnp.int32)
        last = (seen_ref[1, spots[d]] == d).astype(jnp.int32)
        flag_ref[d] = jnp.where(route_ref[d] >= 0, route_ref[d] * 4 + first * 2 + last, -1)
    codes = code_ref[...]
    for d in range(shards):
        match = (codes == code_ref[d : d + 1, :]) & (codes >= 0)
        same_ref[d] = jnp.where(match, 1.0, 0.0)


def own_pass(moves, sub_count, shards, route, queries, keys, values):
    tiles = queries.shape[0]
    return pl.pallas_call(
        functools.partial(own_kernel, moves, sub_count),
        out_shape=(
            jax.ShapeDtypeStruct(queries.shape, jnp.float32),
            jax.ShapeDtypeStruct(queries.shape, jnp.float32),
            jax.ShapeDtypeStruct((shards, LANES), jnp.float32),
            jax.ShapeDtypeStruct((shards, shards, LANES), jnp.float32),
            jax.ShapeDtypeStruct((shards,), jnp.int32),
        ),
        in_specs=[SMEM] + [VMEM] * (1 + 2 * len(moves)),
        out_specs=(VMEM,) * 4 + (SMEM,),
        scratch_shapes=[
            pltpu.VMEM((tiles, KEY_VALUE_HEADS, LANES), jnp.float32),
            pltpu.VMEM((shards, LANES), jnp.int32),
            pltpu.SMEM((2, tiles * KEY_VALUE_HEADS + 1), jnp.int32),
        ],
        compiler_params=PARAMS,
        name="own",
    )(route, queries, *keys, *values)


def others(shards):
    mine = lax.axis_index("ctx")
    return [(mine + 1 + i) % shards for i in range(shards - 1)]


def pick_group(label, wide):
    picked = wide[:, :HEAD_SIZE]
    for g in range(1, KEY_VALUE_HEADS):
        picked = jnp.where(label == g, wide[:, g * HEAD_SIZE : (g + 1) * HEAD_SIZE], picked)
    return picked


def labels_of(packed_ref, slots, body):
    return jnp.concatenate(
        [
            jnp.broadcast_to(packed_ref[pl.ds(j * (body + PAD) + body, 1), :], (body, LANES))
            for j in slots
        ],
        axis=0,
    )


def routed_kernel(count, shards, packed_ref, *refs):
    k_refs, v_refs, reply_ref = refs[:count], refs[count : 2 * count], refs[2 * count]
    span = packed_ref.shape[0] // shards
    body = span - PAD
    slots = others(shards)
    places = [spot_of(j, SEND_LEAD, shards) for j in slots]
    label = labels_of(packed_ref, places, body)
    rows = jnp.concatenate([packed_ref[pl.ds(j * span, body), :] for j in places], axis=0) * SCALE
    wide = jnp.concatenate(
        [jnp.where(label == g, rows, 0.0) for g in range(KEY_VALUE_HEADS)], axis=1
    )
    high, low = halves(wide)
    left = jnp.concatenate([high, low, high], axis=1)
    pieces = []
    for k_ref in k_refs:
        k_high, k_low = halves(k_ref[...])
        pieces.append(dot_nt(left, jnp.concatenate([k_high, k_high, k_low], axis=1)))
    parts = []
    for start in range(0, count, 2):
        some = pieces[start : start + 2]
        top = row_max(some)
        weights = [jnp.exp2(piece - top) for piece in some]
        total = row_sum(weights)
        result = None
        for weight, v_ref in zip(weights, v_refs[start : start + 2]):
            w_high, w_low = halves(weight)
            v_high, v_low = halves(v_ref[...])
            part = dot_nn(w_high, v_high) + dot_nn(w_low, v_high) + dot_nn(w_high, v_low)
            result = part if result is None else result + part
        parts.append((top, total, pick_group(label, result)))
    top = functools.reduce(jnp.maximum, [part[0] for part in parts])
    shrinks = [jnp.exp2(part[0] - top) for part in parts]
    total = sum(shrink * part[1] for shrink, part in zip(shrinks, parts))
    scale = 1.0 / total
    out = sum(shrink * scale * part[2] for shrink, part in zip(shrinks, parts))
    lines = lines_of(top + jnp.log2(total), shards - 1, 0)
    for i, slot in enumerate(slots):
        j = spot_of(slot, REPLY_LEAD, shards)
        reply_ref[pl.ds(j * span, body), :] = out[i * body : (i + 1) * body]
        reply_ref[pl.ds(j * span + body, PAD), :] = jnp.broadcast_to(lines[i : i + 1], (PAD, LANES))


def routed_pass(shards, packed, keys, values):
    count = len(keys)
    return pl.pallas_call(
        functools.partial(routed_kernel, count, shards),
        out_shape=jax.ShapeDtypeStruct(packed.shape, jnp.float32),
        in_specs=[VMEM] * (1 + 2 * count),
        out_specs=VMEM,
        compiler_params=PARAMS,
        name="routed",
    )(packed, *keys, *values)


def merge_kernel(
    flag_vmem, reply_ref, ours_ref, same_ref, _own, _base, own_ref, out_ref, flag_ref, flag_sem, sems
):
    table = pltpu.make_async_copy(flag_vmem, flag_ref, flag_sem)
    table.start()
    rows = own_ref.shape[1]
    body = GROUP * rows
    span = body + PAD
    shards = ours_ref.shape[0]
    width = GROUP * HEAD_SIZE
    ours = ours_ref[...]
    spots = [spot_of(d, REPLY_LEAD, shards) * span for d in range(shards)]
    lines = [reply_ref[spot + body : spot + body + 1, :] for spot in spots]
    match = [same_ref[d] > 0.5 for d in range(shards)]
    top = ours
    for d in range(shards):
        top = jnp.maximum(top, jnp.where(match[d], lines[d], LOW_FILL))
    w_ours = jnp.exp2(ours - top)
    total = w_ours
    for d in range(shards):
        total = total + jnp.where(match[d], jnp.exp2(lines[d] - top), 0.0)
    scale = 1.0 / total
    w_ours = w_ours * scale
    w_theirs = jnp.exp2(jnp.concatenate(lines, axis=0) - top) * scale
    row = lax.broadcasted_iota(jnp.int32, (body, LANES), 0)
    lane = lax.broadcasted_iota(jnp.int32, (body, LANES), 1)

    def stand(line):
        wide = jnp.where(row == lane, jnp.broadcast_to(line, (body, LANES)), 0.0)
        return jnp.sum(wide, axis=1, keepdims=True)

    pairs = [(stand(w_ours[d : d + 1]), stand(w_theirs[d : d + 1])) for d in range(shards)]

    table.wait()
    flags = [flag_ref[d] for d in range(shards)]

    def store(d):
        code = flags[d] // 4
        t = code // KEY_VALUE_HEADS
        columns = pl.ds(pl.multiple_of(code % KEY_VALUE_HEADS * width, width), width)
        return pltpu.make_async_copy(
            own_ref.at[t, :, columns], out_ref.at[t, :, columns], sems.at[d]
        )

    for d in range(shards):

        @pl.when(flags[d] >= 0)
        def _():
            code = flags[d] // 4
            t = code // KEY_VALUE_HEADS
            g = code % KEY_VALUE_HEADS
            a = jnp.where(flags[d] // 2 % 2 == 1, pairs[d][0], 1.0)
            b = pairs[d][1]
            for h in range(GROUP):
                column = pl.ds(pl.multiple_of((g * GROUP + h) * HEAD_SIZE, HEAD_SIZE), HEAD_SIZE)
                part = slice(h * rows, (h + 1) * rows)
                start = spots[d] + h * rows
                own_ref[t, :, column] = (
                    a[part] * own_ref[t, :, column] + b[part] * reply_ref[start : start + rows, :]
                )

            @pl.when(flags[d] % 2 == 1)
            def _():
                store(d).start()

    for d in range(shards):

        @pl.when((flags[d] >= 0) & (flags[d] % 2 == 1))
        def _():
            store(d).wait()


def on_device(queries, keys, values, selected):
    shards = lax.axis_size("ctx")
    sub_count = lax.axis_size("sub")
    tiles, rows, _ = queries.shape
    chips = sub_count // CORES
    span = GROUP * rows + PAD
    keys = keys.reshape(keys.shape[1:])
    values = values.reshape(values.shape[1:])

    def exchange(x, lead):
        order = [int(i) for i in np.argsort([spot_of(d, lead, shards) for d in range(shards)])]
        parted = x.reshape(shards, span // PAD, PAD, LANES)
        moved = lax.all_to_all(
            parted, "ctx", split_axis=0, concat_axis=0, tiled=True, axis_index_groups=[order]
        )
        return moved.reshape(x.shape)

    def swap(x):
        return lax.ppermute(x, "sub", [(s, s ^ 1) for s in range(sub_count)])

    def shift(x, step):
        return lax.ppermute(
            x, "sub", [(s, (s + step * CORES) % sub_count) for s in range(sub_count)]
        )

    far_keys = [shift(keys, step) for step in range(1, chips)]
    far_values = [shift(values, step) for step in range(1, chips)]
    near_keys, near_values = [keys, swap(keys)], [values, swap(values)]

    packed, route = pl.pallas_call(
        pack_kernel,
        out_shape=(
            jax.ShapeDtypeStruct((shards * span, LANES), jnp.float32),
            jax.ShapeDtypeStruct((shards,), jnp.int32),
        ),
        in_specs=[HBM, HBM],
        out_specs=(VMEM, SMEM),
        scratch_shapes=[
            pltpu.SMEM(selected.shape[::-1], jnp.int32),
            pltpu.SMEM((shards + 1,), jnp.int32),
            pltpu.VMEM(queries.shape, jnp.float32),
            pltpu.SemaphoreType.DMA(()),
            pltpu.SemaphoreType.DMA((tiles // 2,)),
        ],
        compiler_params=PARAMS,
        name="pack",
    )(
        pltpu.with_memory_space_constraint(jnp.transpose(selected, (2, 1, 0)), pltpu.HBM),
        pltpu.with_memory_space_constraint(queries, pltpu.HBM),
    )
    arrived = exchange(packed, SEND_LEAD)

    near_moves = ((0, False), (0, True))
    far_moves = tuple((step, swapped) for step in range(1, chips) for swapped in (False, True))
    rest_keys, rest_values = [], []
    for far_key, far_value in zip(far_keys, far_values):
        rest_keys += [far_key, swap(far_key)]
        rest_values += [far_value, swap(far_value)]
    all_keys, all_values = near_keys + rest_keys, near_values + rest_values
    reply = routed_pass(shards, arrived, all_keys, all_values)
    answers = exchange(reply, REPLY_LEAD)
    base, own_out, ours, same, flags = own_pass(
        near_moves + far_moves, sub_count, shards, route, queries, all_keys, all_values
    )
    return pl.pallas_call(
        merge_kernel,
        out_shape=(
            jax.ShapeDtypeStruct(own_out.shape, jnp.float32),
            jax.ShapeDtypeStruct(queries.shape, jnp.float32),
        ),
        in_specs=[VMEM, VMEM, VMEM, VMEM, VMEM, HBM],
        out_specs=(VMEM, HBM),
        input_output_aliases={4: 0, 5: 1},
        scratch_shapes=[
            pltpu.SMEM((shards,), jnp.int32),
            pltpu.SemaphoreType.DMA(()),
            pltpu.SemaphoreType.DMA((shards,)),
        ],
        compiler_params=PARAMS,
        name="merge",
    )(flags, answers, ours, same, own_out, base)[1]


def solution(mesh):
    in_specs = (
        P("ctx", "sub", None),
        P("ctx", "sub", None),
        P("ctx", "sub", None),
        P("ctx", None, None),
    )
    out_specs = P("ctx", "sub", None)

    return jax.shard_map(
        on_device, mesh=mesh, in_specs=in_specs, out_specs=out_specs, check_vma=False
    )
```

```python
import functools
import math

import jax
import jax.numpy as jnp
import numpy as np
from jax import lax
from jax.experimental import pallas as pl
from jax.experimental.pallas import tpu as pltpu
from jax.sharding import PartitionSpec as P


QUERY_HEADS = 4
KEY_VALUE_HEADS = 2
HEAD_SIZE = 128
GROUP = QUERY_HEADS // KEY_VALUE_HEADS
CORES = 2
LANES = 128
PAD = 2
SEND_LEAD = 0.5
REPLY_LEAD = 0.5

LOW_FILL = -1e30
SCALE = HEAD_SIZE ** (-0.5) * math.log2(math.e)


VMEM = pl.BlockSpec(memory_space=pltpu.VMEM)
SMEM = pl.BlockSpec(memory_space=pltpu.SMEM)
HBM = pl.BlockSpec(memory_space=pltpu.HBM)
PARAMS = pltpu.CompilerParams(vmem_limit_bytes=24 * 1024 * 1024)


def spot_of(d, lead, shards):
    return (d + shards - int(lead * shards)) % shards


def halves(x):
    high = x.astype(jnp.bfloat16)
    low = (x - high.astype(jnp.float32)).astype(jnp.bfloat16)
    return high, low


def dot_nt(a, b):
    return lax.dot_general(
        a, b, (((1,), (1,)), ((), ())), preferred_element_type=jnp.float32
    )


def dot_nn(a, b):
    return lax.dot_general(
        a, b, (((1,), (0,)), ((), ())), preferred_element_type=jnp.float32
    )


def find_routes(sel_ref, found_ref):
    picks, groups, tiles = sel_ref.shape
    shards = found_ref.shape[0] - 1
    mine = lax.axis_index("ctx")
    for d in range(shards):
        found_ref[d] = -1
    for t in range(tiles):
        for g in range(groups):
            for c in range(picks):
                d = sel_ref[c, g, t]
                found_ref[jnp.where(d < mine, d, shards)] = t * groups + g


def pack_kernel(
    sel_hbm, q_hbm, packed_ref, sel_ref, found_ref, q_ref, sel_sem, q_sem
):
    table = pltpu.make_async_copy(sel_hbm, sel_ref, sel_sem)
    table.start()
    tiles, rows, _ = q_ref.shape
    fetches = [
        pltpu.make_async_copy(q_hbm.at[pl.ds(t, 2)], q_ref.at[pl.ds(t, 2)], q_sem.at[t // 2])
        for t in range(0, tiles, 2)
    ]
    for fetch in fetches:
        fetch.start()
    span = GROUP * rows + PAD
    shards = packed_ref.shape[0] // span
    table.wait()
    find_routes(sel_ref, found_ref)
    for fetch in fetches:
        fetch.wait()

    for d in range(shards):
        code = jnp.maximum(found_ref[d], 0)
        t = code // KEY_VALUE_HEADS
        g = code % KEY_VALUE_HEADS
        for h in range(GROUP):
            column = pl.multiple_of((g * GROUP + h) * HEAD_SIZE, HEAD_SIZE)
            start = spot_of(d, SEND_LEAD, shards) * span + h * rows
            packed_ref[start : start + rows, :] = q_ref[t, :, pl.ds(column, HEAD_SIZE)]
        label = jnp.full((PAD, LANES), g, jnp.int32).astype(jnp.float32)
        end = (spot_of(d, SEND_LEAD, shards) + 1) * span
        packed_ref[end - PAD : end, :] = label


def source_of(sub, move, sub_count):
    step, swapped = move
    source = (sub - step * CORES + sub_count) % sub_count
    return source ^ 1 if swapped else source


def own_scores(offsets, sub_count, q_ref, k_refs, head_pair):
    tiles, rows, _ = q_ref.shape
    per_head = tiles * rows
    key_rows = k_refs[0].shape[0]
    sub = lax.axis_index("sub")
    tile_span = rows * sub_count
    q = jnp.concatenate(
        [
            q_ref[:, :, (head_pair * GROUP + h) * HEAD_SIZE : (head_pair * GROUP + h + 1) * HEAD_SIZE]
            .reshape(per_head, HEAD_SIZE)
            for h in range(GROUP)
        ],
        axis=0,
    )
    high, low = halves(q * SCALE)
    left = jnp.concatenate([high, low, high, low], axis=1)
    row = lax.broadcasted_iota(jnp.int32, (GROUP * per_head, key_rows), 0) % per_head
    row = row // rows * tile_span + row % rows + sub * rows
    column = lax.broadcasted_iota(jnp.int32, (GROUP * per_head, key_rows), 1)
    gap = column - row
    pieces = []
    for k_ref, offset in zip(k_refs, offsets):
        k_high, k_low = halves(k_ref[:, head_pair * HEAD_SIZE : (head_pair + 1) * HEAD_SIZE])
        right = jnp.concatenate([k_high, k_high, k_low, k_low], axis=1)
        score = dot_nt(left, right)
        pieces.append(jnp.where(gap <= -offset * key_rows, score, LOW_FILL))
    return pieces


def row_max(pieces):
    top = pieces[0]
    for piece in pieces[1:]:
        top = jnp.maximum(top, piece)
    return jnp.max(top, axis=1, keepdims=True)


def row_sum(pieces):
    total = pieces[0]
    for piece in pieces[1:]:
        total = total + piece
    return jnp.sum(total, axis=1, keepdims=True)


def own_values(weights, v_refs, head_pair):
    total = None
    for weight, v_ref in zip(weights, v_refs):
        w_high, w_low = halves(weight)
        v_high, v_low = halves(v_ref[:, head_pair * HEAD_SIZE : (head_pair + 1) * HEAD_SIZE])
        right = jnp.concatenate([v_high, v_low], axis=1)
        part = dot_nn(w_high, right) + dot_nn(w_low, right)
        total = part if total is None else total + part
    return total[:, :HEAD_SIZE] + total[:, HEAD_SIZE:]


def lines_of(lse, blocks, rows):
    height = lse.shape[0] // blocks
    wide = jnp.broadcast_to(lse, (lse.shape[0], LANES)).reshape(blocks, height, LANES)
    row = lax.broadcasted_iota(jnp.int32, wide.shape, 1)
    lane = lax.broadcasted_iota(jnp.int32, wide.shape, 2)
    return jnp.sum(jnp.where(row == lane - rows, wide, 0.0), axis=1)


def own_kernel(moves, sub_count, sel_hbm, q_ref, *refs):
    count = len(moves)
    k_refs, v_refs, rest = refs[:count], refs[count : 2 * count], refs[2 * count :]
    base_ref, out_ref, ours_ref, same_ref, flag_ref, *scratch = rest
    lse_ref, code_ref, seen_ref, sel_ref, route_ref, sel_sem = scratch
    table = pltpu.make_async_copy(sel_hbm, sel_ref, sel_sem)
    table.start()
    tiles, rows, _ = q_ref.shape
    per_head = tiles * rows
    sub = lax.axis_index("sub")
    offsets = [source_of(sub, move, sub_count) for move in moves]
    for g in range(KEY_VALUE_HEADS):
        pieces = own_scores(offsets, sub_count, q_ref, k_refs, g)
        top = row_max(pieces)
        weights = [jnp.exp2(piece - top) for piece in pieces]
        total = row_sum(weights)
        out = own_values(weights, v_refs, g) / total
        lse = top + jnp.log2(total)
        lines = None
        for h in range(GROUP):
            column = (g * GROUP + h) * HEAD_SIZE
            span = slice(h * per_head, (h + 1) * per_head)
            block = out[span].reshape(tiles, rows, HEAD_SIZE)
            base_ref[:, :, column : column + HEAD_SIZE] = block
            out_ref[:, :, column : column + HEAD_SIZE] = block
            part = lines_of(lse[span], tiles, h * rows)
            lines = part if lines is None else lines + part
        lse_ref[:, g, :] = lines


    table.wait()
    find_routes(sel_ref, route_ref)
    shards = ours_ref.shape[0]
    blank = seen_ref.shape[1] - 1
    spots = []
    for d in range(shards):
        code = route_ref[d]
        code_ref[d : d + 1, :] = jnp.full((1, LANES), code, jnp.int32)
        t = jnp.maximum(code, 0) // KEY_VALUE_HEADS
        g = jnp.maximum(code, 0) % KEY_VALUE_HEADS
        ours_ref[d : d + 1, :] = lse_ref[t, pl.ds(g, 1), :]
        spots.append(jnp.where(code >= 0, code, blank))
    for d in range(shards):
        seen_ref[0, spots[shards - 1 - d]] = shards - 1 - d
        seen_ref[1, spots[d]] = d
    for d in range(shards):
        first = (seen_ref[0, spots[d]] == d).astype(jnp.int32)
        last = (seen_ref[1, spots[d]] == d).astype(jnp.int32)
        flag_ref[d] = jnp.where(route_ref[d] >= 0, route_ref[d] * 4 + first * 2 + last, -1)
    codes = code_ref[...]
    for d in range(shards):
        match = (codes == code_ref[d : d + 1, :]) & (codes >= 0)
        same_ref[d] = jnp.where(match, 1.0, 0.0)


def own_pass(moves, sub_count, shards, table, queries, keys, values):
    tiles = queries.shape[0]
    return pl.pallas_call(
        functools.partial(own_kernel, moves, sub_count),
        out_shape=(
            jax.ShapeDtypeStruct(queries.shape, jnp.float32),
            jax.ShapeDtypeStruct(queries.shape, jnp.float32),
            jax.ShapeDtypeStruct((shards, LANES), jnp.float32),
            jax.ShapeDtypeStruct((shards, shards, LANES), jnp.float32),
            jax.ShapeDtypeStruct((shards,), jnp.int32),
        ),
        in_specs=[HBM] + [VMEM] * (1 + 2 * len(moves)),
        out_specs=(VMEM,) * 4 + (SMEM,),
        scratch_shapes=[
            pltpu.VMEM((tiles, KEY_VALUE_HEADS, LANES), jnp.float32),
            pltpu.VMEM((shards, LANES), jnp.int32),
            pltpu.SMEM((2, tiles * KEY_VALUE_HEADS + 1), jnp.int32),
            pltpu.SMEM(table.shape, jnp.int32),
            pltpu.SMEM((shards + 1,), jnp.int32),
            pltpu.SemaphoreType.DMA(()),
        ],
        compiler_params=PARAMS,
        name="own",
    )(table, queries, *keys, *values)


def others(shards):
    mine = lax.axis_index("ctx")
    return [(mine + 1 + i) % shards for i in range(shards - 1)]


def pick_group(label, wide):
    picked = wide[:, :HEAD_SIZE]
    for g in range(1, KEY_VALUE_HEADS):
        picked = jnp.where(label == g, wide[:, g * HEAD_SIZE : (g + 1) * HEAD_SIZE], picked)
    return picked


def labels_of(packed_ref, slots, body):
    return jnp.concatenate(
        [
            jnp.broadcast_to(packed_ref[pl.ds(j * (body + PAD) + body, 1), :], (body, LANES))
            for j in slots
        ],
        axis=0,
    )


def routed_kernel(count, shards, packed_ref, *refs):
    k_refs, v_refs, reply_ref = refs[:count], refs[count : 2 * count], refs[2 * count]
    span = packed_ref.shape[0] // shards
    body = span - PAD
    slots = others(shards)
    places = [spot_of(j, SEND_LEAD, shards) for j in slots]
    label = labels_of(packed_ref, places, body)
    rows = jnp.concatenate([packed_ref[pl.ds(j * span, body), :] for j in places], axis=0) * SCALE
    wide = jnp.concatenate(
        [jnp.where(label == g, rows, 0.0) for g in range(KEY_VALUE_HEADS)], axis=1
    )
    high, low = halves(wide)
    left = jnp.concatenate([high, low, high], axis=1)
    pieces = []
    for k_ref in k_refs:
        k_high, k_low = halves(k_ref[...])
        pieces.append(dot_nt(left, jnp.concatenate([k_high, k_high, k_low], axis=1)))
    parts = []
    for start in range(0, count, 2):
        some = pieces[start : start + 2]
        top = row_max(some)
        weights = [jnp.exp2(piece - top) for piece in some]
        total = row_sum(weights)
        result = None
        for weight, v_ref in zip(weights, v_refs[start : start + 2]):
            w_high, w_low = halves(weight)
            v_high, v_low = halves(v_ref[...])
            part = dot_nn(w_high, v_high) + dot_nn(w_low, v_high) + dot_nn(w_high, v_low)
            result = part if result is None else result + part
        parts.append((top, total, pick_group(label, result)))
    top = functools.reduce(jnp.maximum, [part[0] for part in parts])
    shrinks = [jnp.exp2(part[0] - top) for part in parts]
    total = sum(shrink * part[1] for shrink, part in zip(shrinks, parts))
    scale = 1.0 / total
    out = sum(shrink * scale * part[2] for shrink, part in zip(shrinks, parts))
    lines = lines_of(top + jnp.log2(total), shards - 1, 0)
    for i, slot in enumerate(slots):
        j = spot_of(slot, REPLY_LEAD, shards)
        reply_ref[pl.ds(j * span, body), :] = out[i * body : (i + 1) * body]
        reply_ref[pl.ds(j * span + body, PAD), :] = jnp.broadcast_to(lines[i : i + 1], (PAD, LANES))


def routed_pass(shards, packed, keys, values):
    count = len(keys)
    return pl.pallas_call(
        functools.partial(routed_kernel, count, shards),
        out_shape=jax.ShapeDtypeStruct(packed.shape, jnp.float32),
        in_specs=[VMEM] * (1 + 2 * count),
        out_specs=VMEM,
        compiler_params=PARAMS,
        name="routed",
    )(packed, *keys, *values)


def merge_kernel(
    flag_vmem, reply_ref, ours_ref, same_ref, _own, _base, own_ref, out_ref, flag_ref, flag_sem, sems
):
    table = pltpu.make_async_copy(flag_vmem, flag_ref, flag_sem)
    table.start()
    rows = own_ref.shape[1]
    body = GROUP * rows
    span = body + PAD
    shards = ours_ref.shape[0]
    width = GROUP * HEAD_SIZE
    ours = ours_ref[...]
    spots = [spot_of(d, REPLY_LEAD, shards) * span for d in range(shards)]
    lines = [reply_ref[spot + body : spot + body + 1, :] for spot in spots]
    match = [same_ref[d] > 0.5 for d in range(shards)]
    top = ours
    for d in range(shards):
        top = jnp.maximum(top, jnp.where(match[d], lines[d], LOW_FILL))
    w_ours = jnp.exp2(ours - top)
    total = w_ours
    for d in range(shards):
        total = total + jnp.where(match[d], jnp.exp2(lines[d] - top), 0.0)
    scale = 1.0 / total
    w_ours = w_ours * scale
    w_theirs = jnp.exp2(jnp.concatenate(lines, axis=0) - top) * scale
    row = lax.broadcasted_iota(jnp.int32, (body, LANES), 0)
    lane = lax.broadcasted_iota(jnp.int32, (body, LANES), 1)

    def stand(line):
        wide = jnp.where(row == lane, jnp.broadcast_to(line, (body, LANES)), 0.0)
        return jnp.sum(wide, axis=1, keepdims=True)

    pairs = [(stand(w_ours[d : d + 1]), stand(w_theirs[d : d + 1])) for d in range(shards)]

    table.wait()
    flags = [flag_ref[d] for d in range(shards)]

    def store(d):
        code = flags[d] // 4
        t = code // KEY_VALUE_HEADS
        columns = pl.ds(pl.multiple_of(code % KEY_VALUE_HEADS * width, width), width)
        return pltpu.make_async_copy(
            own_ref.at[t, :, columns], out_ref.at[t, :, columns], sems.at[d]
        )

    for d in range(shards):

        @pl.when(flags[d] >= 0)
        def _():
            code = flags[d] // 4
            t = code // KEY_VALUE_HEADS
            g = code % KEY_VALUE_HEADS
            a = jnp.where(flags[d] // 2 % 2 == 1, pairs[d][0], 1.0)
            b = pairs[d][1]
            for h in range(GROUP):
                column = pl.ds(pl.multiple_of((g * GROUP + h) * HEAD_SIZE, HEAD_SIZE), HEAD_SIZE)
                part = slice(h * rows, (h + 1) * rows)
                start = spots[d] + h * rows
                own_ref[t, :, column] = (
                    a[part] * own_ref[t, :, column] + b[part] * reply_ref[start : start + rows, :]
                )

            @pl.when(flags[d] % 2 == 1)
            def _():
                store(d).start()

    for d in range(shards):

        @pl.when((flags[d] >= 0) & (flags[d] % 2 == 1))
        def _():
            store(d).wait()


def on_device(queries, keys, values, selected):
    shards = lax.axis_size("ctx")
    sub_count = lax.axis_size("sub")
    tiles, rows, _ = queries.shape
    chips = sub_count // CORES
    span = GROUP * rows + PAD
    keys = keys.reshape(keys.shape[1:])
    values = values.reshape(values.shape[1:])

    def exchange(x, lead):
        order = [int(i) for i in np.argsort([spot_of(d, lead, shards) for d in range(shards)])]
        parted = x.reshape(shards, span // PAD, PAD, LANES)
        moved = lax.all_to_all(
            parted, "ctx", split_axis=0, concat_axis=0, tiled=True, axis_index_groups=[order]
        )
        return moved.reshape(x.shape)

    def swap(x):
        return lax.ppermute(x, "sub", [(s, s ^ 1) for s in range(sub_count)])

    def shift(x, step):
        return lax.ppermute(
            x, "sub", [(s, (s + step * CORES) % sub_count) for s in range(sub_count)]
        )

    far_keys = [shift(keys, step) for step in range(1, chips)]
    far_values = [shift(values, step) for step in range(1, chips)]
    near_keys, near_values = [keys, swap(keys)], [values, swap(values)]

    table = pltpu.with_memory_space_constraint(jnp.transpose(selected, (2, 1, 0)), pltpu.HBM)
    packed = pl.pallas_call(
        pack_kernel,
        out_shape=jax.ShapeDtypeStruct((shards * span, LANES), jnp.float32),
        in_specs=[HBM, HBM],
        out_specs=VMEM,
        scratch_shapes=[
            pltpu.SMEM(selected.shape[::-1], jnp.int32),
            pltpu.SMEM((shards + 1,), jnp.int32),
            pltpu.VMEM(queries.shape, jnp.float32),
            pltpu.SemaphoreType.DMA(()),
            pltpu.SemaphoreType.DMA((tiles // 2,)),
        ],
        compiler_params=PARAMS,
        name="pack",
    )(
        table,
        pltpu.with_memory_space_constraint(queries, pltpu.HBM),
    )
    arrived = exchange(packed, SEND_LEAD)

    near_moves = ((0, False), (0, True))
    far_moves = tuple((step, swapped) for step in range(1, chips) for swapped in (False, True))
    rest_keys, rest_values = [], []
    for far_key, far_value in zip(far_keys, far_values):
        rest_keys += [far_key, swap(far_key)]
        rest_values += [far_value, swap(far_value)]
    all_keys, all_values = near_keys + rest_keys, near_values + rest_values
    reply = routed_pass(shards, arrived, all_keys, all_values)
    answers = exchange(reply, REPLY_LEAD)
    base, own_out, ours, same, flags = own_pass(
        near_moves + far_moves, sub_count, shards, table, queries, all_keys, all_values
    )
    return pl.pallas_call(
        merge_kernel,
        out_shape=(
            jax.ShapeDtypeStruct(own_out.shape, jnp.float32),
            jax.ShapeDtypeStruct(queries.shape, jnp.float32),
        ),
        in_specs=[VMEM, VMEM, VMEM, VMEM, VMEM, HBM],
        out_specs=(VMEM, HBM),
        input_output_aliases={4: 0, 5: 1},
        scratch_shapes=[
            pltpu.SMEM((shards,), jnp.int32),
            pltpu.SemaphoreType.DMA(()),
            pltpu.SemaphoreType.DMA((shards,)),
        ],
        compiler_params=PARAMS,
        name="merge",
    )(flags, answers, ours, same, own_out, base)[1]


def solution(mesh):
    in_specs = (
        P("ctx", "sub", None),
        P("ctx", "sub", None),
        P("ctx", "sub", None),
        P("ctx", None, None),
    )
    out_specs = P("ctx", "sub", None)

    return jax.shard_map(
        on_device, mesh=mesh, in_specs=in_specs, out_specs=out_specs, check_vma=False
    )
```

```python
import functools
import math

import jax
import jax.numpy as jnp
import numpy as np
from jax import lax
from jax.experimental import pallas as pl
from jax.experimental.pallas import tpu as pltpu
from jax.sharding import PartitionSpec as P


QUERY_HEADS = 4
KEY_VALUE_HEADS = 2
HEAD_SIZE = 128
GROUP = QUERY_HEADS // KEY_VALUE_HEADS
CORES = 2
LANES = 128
PAD = 2
SEND_LEAD = 0.5
REPLY_LEAD = 0.5

LOW_FILL = -1e30
SCALE = HEAD_SIZE ** (-0.5) * math.log2(math.e)


VMEM = pl.BlockSpec(memory_space=pltpu.VMEM)
SMEM = pl.BlockSpec(memory_space=pltpu.SMEM)
HBM = pl.BlockSpec(memory_space=pltpu.HBM)
PARAMS = pltpu.CompilerParams(vmem_limit_bytes=24 * 1024 * 1024)


def spot_of(d, lead, shards):
    return (d + shards - int(lead * shards)) % shards


def halves(x):
    high = x.astype(jnp.bfloat16)
    low = (x - high.astype(jnp.float32)).astype(jnp.bfloat16)
    return high, low


def dot_nt(a, b):
    return lax.dot_general(
        a, b, (((1,), (1,)), ((), ())), preferred_element_type=jnp.float32
    )


def dot_nn(a, b):
    return lax.dot_general(
        a, b, (((1,), (0,)), ((), ())), preferred_element_type=jnp.float32
    )


def find_routes(sel_ref, found_ref):
    picks, groups, tiles = sel_ref.shape
    shards = found_ref.shape[0] - 1
    mine = lax.axis_index("ctx")
    for d in range(shards):
        found_ref[d] = -1
    for t in range(tiles):
        for g in range(groups):
            for c in range(picks):
                d = sel_ref[c, g, t]
                found_ref[jnp.where(d < mine, d, shards)] = t * groups + g


def pack_kernel(
    sel_hbm, q_hbm, packed_ref, sel_ref, found_ref, q_ref, sel_sem, q_sem
):
    table = pltpu.make_async_copy(sel_hbm, sel_ref, sel_sem)
    table.start()
    tiles, rows, _ = q_ref.shape
    fetches = [
        pltpu.make_async_copy(q_hbm.at[pl.ds(t, 2)], q_ref.at[pl.ds(t, 2)], q_sem.at[t // 2])
        for t in range(0, tiles, 2)
    ]
    for fetch in fetches:
        fetch.start()
    span = GROUP * rows + PAD
    shards = packed_ref.shape[0] // span
    table.wait()
    find_routes(sel_ref, found_ref)
    for fetch in fetches:
        fetch.wait()

    for d in range(shards):
        code = jnp.maximum(found_ref[d], 0)
        t = code // KEY_VALUE_HEADS
        g = code % KEY_VALUE_HEADS
        for h in range(GROUP):
            column = pl.multiple_of((g * GROUP + h) * HEAD_SIZE, HEAD_SIZE)
            start = spot_of(d, SEND_LEAD, shards) * span + h * rows
            packed_ref[start : start + rows, :] = q_ref[t, :, pl.ds(column, HEAD_SIZE)]
        label = jnp.full((PAD, LANES), g, jnp.int32).astype(jnp.float32)
        end = (spot_of(d, SEND_LEAD, shards) + 1) * span
        packed_ref[end - PAD : end, :] = label


def source_of(sub, move, sub_count):
    step, swapped = move
    source = (sub - step * CORES + sub_count) % sub_count
    return source ^ 1 if swapped else source


def own_scores(offsets, sub_count, q_ref, k_refs, head_pair):
    tiles, rows, _ = q_ref.shape
    per_head = tiles * rows
    key_rows = k_refs[0].shape[0]
    sub = lax.axis_index("sub")
    tile_span = rows * sub_count
    q = jnp.concatenate(
        [
            q_ref[:, :, (head_pair * GROUP + h) * HEAD_SIZE : (head_pair * GROUP + h + 1) * HEAD_SIZE]
            .reshape(per_head, HEAD_SIZE)
            for h in range(GROUP)
        ],
        axis=0,
    )
    high, low = halves(q * SCALE)
    left = jnp.concatenate([high, low, high, low], axis=1)
    row = lax.broadcasted_iota(jnp.int32, (GROUP * per_head, key_rows), 0) % per_head
    row = row // rows * tile_span + row % rows + sub * rows
    column = lax.broadcasted_iota(jnp.int32, (GROUP * per_head, key_rows), 1)
    gap = column - row
    pieces = []
    for k_ref, offset in zip(k_refs, offsets):
        k_high, k_low = halves(k_ref[:, head_pair * HEAD_SIZE : (head_pair + 1) * HEAD_SIZE])
        right = jnp.concatenate([k_high, k_high, k_low, k_low], axis=1)
        score = dot_nt(left, right)
        pieces.append(jnp.where(gap <= -offset * key_rows, score, LOW_FILL))
    return pieces


def row_max(pieces):
    top = pieces[0]
    for piece in pieces[1:]:
        top = jnp.maximum(top, piece)
    return jnp.max(top, axis=1, keepdims=True)


def row_sum(pieces):
    total = pieces[0]
    for piece in pieces[1:]:
        total = total + piece
    return jnp.sum(total, axis=1, keepdims=True)


def own_values(weights, v_refs, head_pair):
    total = None
    for weight, v_ref in zip(weights, v_refs):
        w_high, w_low = halves(weight)
        v_high, v_low = halves(v_ref[:, head_pair * HEAD_SIZE : (head_pair + 1) * HEAD_SIZE])
        right = jnp.concatenate([v_high, v_low], axis=1)
        part = dot_nn(w_high, right) + dot_nn(w_low, right)
        total = part if total is None else total + part
    return total[:, :HEAD_SIZE] + total[:, HEAD_SIZE:]


def lines_of(lse, blocks, rows):
    height = lse.shape[0] // blocks
    wide = jnp.broadcast_to(lse, (lse.shape[0], LANES)).reshape(blocks, height, LANES)
    row = lax.broadcasted_iota(jnp.int32, wide.shape, 1)
    lane = lax.broadcasted_iota(jnp.int32, wide.shape, 2)
    return jnp.sum(jnp.where(row == lane - rows, wide, 0.0), axis=1)


def own_kernel(moves, sub_count, sel_hbm, q_ref, *refs):
    count = len(moves)
    k_refs, v_refs, rest = refs[:count], refs[count : 2 * count], refs[2 * count :]
    base_ref, out_ref, ours_ref, same_ref, flag_ref, *scratch = rest
    lse_ref, code_ref, seen_ref, sel_ref, route_ref, sel_sem = scratch
    table = pltpu.make_async_copy(sel_hbm, sel_ref, sel_sem)
    table.start()
    tiles, rows, _ = q_ref.shape
    per_head = tiles * rows
    sub = lax.axis_index("sub")
    offsets = [source_of(sub, move, sub_count) for move in moves]
    for g in range(KEY_VALUE_HEADS):
        pieces = own_scores(offsets, sub_count, q_ref, k_refs, g)
        top = row_max(pieces)
        weights = [jnp.exp2(piece - top) for piece in pieces]
        total = row_sum(weights)
        out = own_values(weights, v_refs, g) / total
        lse = top + jnp.log2(total)
        lines = None
        for h in range(GROUP):
            column = (g * GROUP + h) * HEAD_SIZE
            span = slice(h * per_head, (h + 1) * per_head)
            block = out[span].reshape(tiles, rows, HEAD_SIZE)
            base_ref[:, :, column : column + HEAD_SIZE] = block
            out_ref[:, :, column : column + HEAD_SIZE] = block
            part = lines_of(lse[span], tiles, h * rows)
            lines = part if lines is None else lines + part
        lse_ref[:, g, :] = lines


    table.wait()
    find_routes(sel_ref, route_ref)
    shards = ours_ref.shape[0]
    blank = seen_ref.shape[1] - 1
    spots = []
    for d in range(shards):
        code = route_ref[d]
        code_ref[d : d + 1, :] = jnp.full((1, LANES), code, jnp.int32)
        t = jnp.maximum(code, 0) // KEY_VALUE_HEADS
        g = jnp.maximum(code, 0) % KEY_VALUE_HEADS
        ours_ref[d : d + 1, :] = lse_ref[t, pl.ds(g, 1), :]
        spots.append(jnp.where(code >= 0, code, blank))
    for d in range(shards):
        seen_ref[0, spots[shards - 1 - d]] = shards - 1 - d
        seen_ref[1, spots[d]] = d
    for d in range(shards):
        first = (seen_ref[0, spots[d]] == d).astype(jnp.int32)
        last = (seen_ref[1, spots[d]] == d).astype(jnp.int32)
        flag_ref[d] = jnp.where(route_ref[d] >= 0, route_ref[d] * 4 + first * 2 + last, -1)
    codes = code_ref[...]
    for d in range(shards):
        match = (codes == code_ref[d : d + 1, :]) & (codes >= 0)
        same_ref[d] = jnp.where(match, 1.0, 0.0)


def own_pass(moves, sub_count, shards, table, queries, keys, values):
    tiles = queries.shape[0]
    return pl.pallas_call(
        functools.partial(own_kernel, moves, sub_count),
        out_shape=(
            jax.ShapeDtypeStruct(queries.shape, jnp.float32),
            jax.ShapeDtypeStruct(queries.shape, jnp.float32),
            jax.ShapeDtypeStruct((shards, LANES), jnp.float32),
            jax.ShapeDtypeStruct((shards, shards, LANES), jnp.float32),
            jax.ShapeDtypeStruct((shards,), jnp.int32),
        ),
        in_specs=[HBM] + [VMEM] * (1 + 2 * len(moves)),
        out_specs=(VMEM,) * 4 + (SMEM,),
        scratch_shapes=[
            pltpu.VMEM((tiles, KEY_VALUE_HEADS, LANES), jnp.float32),
            pltpu.VMEM((shards, LANES), jnp.int32),
            pltpu.SMEM((2, tiles * KEY_VALUE_HEADS + 1), jnp.int32),
            pltpu.SMEM(table.shape, jnp.int32),
            pltpu.SMEM((shards + 1,), jnp.int32),
            pltpu.SemaphoreType.DMA(()),
        ],
        compiler_params=PARAMS,
        name="own",
    )(table, queries, *keys, *values)


def others(shards):
    mine = lax.axis_index("ctx")
    return [(mine + 1 + i) % shards for i in range(shards - 1)]


def pick_group(label, wide):
    picked = wide[:, :HEAD_SIZE]
    for g in range(1, KEY_VALUE_HEADS):
        picked = jnp.where(label == g, wide[:, g * HEAD_SIZE : (g + 1) * HEAD_SIZE], picked)
    return picked


def labels_of(packed_ref, slots, body):
    return jnp.concatenate(
        [
            jnp.broadcast_to(packed_ref[pl.ds(j * (body + PAD) + body, 1), :], (body, LANES))
            for j in slots
        ],
        axis=0,
    )


def routed_kernel(count, shards, packed_ref, *refs):
    k_refs, v_refs, reply_ref = refs[:count], refs[count : 2 * count], refs[2 * count]
    span = packed_ref.shape[0] // shards
    body = span - PAD
    slots = others(shards)
    places = [spot_of(j, SEND_LEAD, shards) for j in slots]
    label = labels_of(packed_ref, places, body)
    rows = jnp.concatenate([packed_ref[pl.ds(j * span, body), :] for j in places], axis=0) * SCALE
    wide = jnp.concatenate(
        [jnp.where(label == g, rows, 0.0) for g in range(KEY_VALUE_HEADS)], axis=1
    )
    high, low = halves(wide)
    left = jnp.concatenate([high, low, high], axis=1)
    pieces = []
    for k_ref in k_refs:
        k_high, k_low = halves(k_ref[...])
        pieces.append(dot_nt(left, jnp.concatenate([k_high, k_high, k_low], axis=1)))
    parts = []
    for start in range(0, count, 2):
        some = pieces[start : start + 2]
        top = row_max(some)
        weights = [jnp.exp2(piece - top) for piece in some]
        total = row_sum(weights)
        result = None
        for weight, v_ref in zip(weights, v_refs[start : start + 2]):
            w_high, w_low = halves(weight)
            v_high, v_low = halves(v_ref[...])
            part = dot_nn(w_high, v_high) + dot_nn(w_low, v_high) + dot_nn(w_high, v_low)
            result = part if result is None else result + part
        parts.append((top, total, pick_group(label, result)))
    top = functools.reduce(jnp.maximum, [part[0] for part in parts])
    shrinks = [jnp.exp2(part[0] - top) for part in parts]
    total = sum(shrink * part[1] for shrink, part in zip(shrinks, parts))
    scale = 1.0 / total
    out = sum(shrink * scale * part[2] for shrink, part in zip(shrinks, parts))
    lines = lines_of(top + jnp.log2(total), shards - 1, 0)
    for i, slot in enumerate(slots):
        j = spot_of(slot, REPLY_LEAD, shards)
        reply_ref[pl.ds(j * span, body), :] = out[i * body : (i + 1) * body]
        reply_ref[pl.ds(j * span + body, PAD), :] = jnp.broadcast_to(lines[i : i + 1], (PAD, LANES))


def routed_pass(shards, packed, keys, values):
    count = len(keys)
    return pl.pallas_call(
        functools.partial(routed_kernel, count, shards),
        out_shape=jax.ShapeDtypeStruct(packed.shape, jnp.float32),
        in_specs=[VMEM] * (1 + 2 * count),
        out_specs=VMEM,
        compiler_params=PARAMS,
        name="routed",
    )(packed, *keys, *values)


def merge_kernel(
    flag_vmem, reply_ref, ours_ref, same_ref, _own, _base, own_ref, out_ref, flag_ref, flag_sem, sems
):
    table = pltpu.make_async_copy(flag_vmem, flag_ref, flag_sem)
    table.start()
    rows = own_ref.shape[1]
    body = GROUP * rows
    span = body + PAD
    shards = ours_ref.shape[0]
    width = GROUP * HEAD_SIZE
    ours = ours_ref[...]
    spots = [spot_of(d, REPLY_LEAD, shards) * span for d in range(shards)]
    lines = [reply_ref[spot + body : spot + body + 1, :] for spot in spots]
    match = [same_ref[d] > 0.5 for d in range(shards)]
    top = ours
    for d in range(shards):
        top = jnp.maximum(top, jnp.where(match[d], lines[d], LOW_FILL))
    w_ours = jnp.exp2(ours - top)
    total = w_ours
    for d in range(shards):
        total = total + jnp.where(match[d], jnp.exp2(lines[d] - top), 0.0)
    scale = 1.0 / total
    w_ours = w_ours * scale
    w_theirs = jnp.exp2(jnp.concatenate(lines, axis=0) - top) * scale
    row = lax.broadcasted_iota(jnp.int32, (body, LANES), 0)
    lane = lax.broadcasted_iota(jnp.int32, (body, LANES), 1)

    def stand(line):
        wide = jnp.where(row == lane, jnp.broadcast_to(line, (body, LANES)), 0.0)
        return jnp.sum(wide, axis=1, keepdims=True)

    pairs = [(stand(w_ours[d : d + 1]), stand(w_theirs[d : d + 1])) for d in range(shards)]

    table.wait()
    flags = [flag_ref[d] for d in range(shards)]

    def store(d):
        code = flags[d] // 4
        t = code // KEY_VALUE_HEADS
        columns = pl.ds(pl.multiple_of(code % KEY_VALUE_HEADS * width, width), width)
        return pltpu.make_async_copy(
            own_ref.at[t, :, columns], out_ref.at[t, :, columns], sems.at[d]
        )

    for d in range(shards):

        @pl.when(flags[d] >= 0)
        def _():
            code = flags[d] // 4
            t = code // KEY_VALUE_HEADS
            g = code % KEY_VALUE_HEADS
            a = jnp.where(flags[d] // 2 % 2 == 1, pairs[d][0], 1.0)
            b = pairs[d][1]
            for h in range(GROUP):
                column = pl.ds(pl.multiple_of((g * GROUP + h) * HEAD_SIZE, HEAD_SIZE), HEAD_SIZE)
                part = slice(h * rows, (h + 1) * rows)
                start = spots[d] + h * rows
                own_ref[t, :, column] = (
                    a[part] * own_ref[t, :, column] + b[part] * reply_ref[start : start + rows, :]
                )

            @pl.when(flags[d] % 2 == 1)
            def _():
                store(d).start()

    for d in range(shards):

        @pl.when((flags[d] >= 0) & (flags[d] % 2 == 1))
        def _():
            store(d).wait()


def on_device(queries, keys, values, selected):
    shards = lax.axis_size("ctx")
    sub_count = lax.axis_size("sub")
    tiles, rows, _ = queries.shape
    chips = sub_count // CORES
    span = GROUP * rows + PAD
    keys = keys.reshape(keys.shape[1:])
    values = values.reshape(values.shape[1:])

    def exchange(x, lead):
        order = [int(i) for i in np.argsort([spot_of(d, lead, shards) for d in range(shards)])]
        parted = x.reshape(shards, span // PAD, PAD, LANES)
        moved = lax.all_to_all(
            parted, "ctx", split_axis=0, concat_axis=0, tiled=True, axis_index_groups=[order]
        )
        return moved.reshape(x.shape)

    def swap(x):
        return lax.ppermute(x, "sub", [(s, s ^ 1) for s in range(sub_count)])

    def shift(x, step):
        return lax.ppermute(
            x, "sub", [(s, (s + step * CORES) % sub_count) for s in range(sub_count)]
        )

    far_keys = [shift(keys, step) for step in range(1, chips)]
    far_values = [shift(values, step) for step in range(1, chips)]
    near_keys, near_values = [keys, swap(keys)], [values, swap(values)]

    table = pltpu.with_memory_space_constraint(jnp.transpose(selected, (2, 1, 0)), pltpu.HBM)
    pack = pl.pallas_call(
        pack_kernel,
        out_shape=jax.ShapeDtypeStruct((shards * span, LANES), jnp.float32),
        in_specs=[HBM, HBM],
        out_specs=VMEM,
        scratch_shapes=[
            pltpu.SMEM(selected.shape[::-1], jnp.int32),
            pltpu.SMEM((shards + 1,), jnp.int32),
            pltpu.VMEM(queries.shape, jnp.float32),
            pltpu.SemaphoreType.DMA(()),
            pltpu.SemaphoreType.DMA((tiles // 2,)),
        ],
        compiler_params=PARAMS,
        name="pack",
    )
    packed = pack(table, pltpu.with_memory_space_constraint(queries, pltpu.HBM))
    arrived = exchange(packed, SEND_LEAD)

    near_moves = ((0, False), (0, True))
    far_moves = tuple((step, swapped) for step in range(1, chips) for swapped in (False, True))
    rest_keys, rest_values = [], []
    for far_key, far_value in zip(far_keys, far_values):
        rest_keys += [far_key, swap(far_key)]
        rest_values += [far_value, swap(far_value)]
    all_keys, all_values = near_keys + rest_keys, near_values + rest_values
    reply = routed_pass(shards, arrived, all_keys, all_values)
    answers = exchange(reply, REPLY_LEAD)
    base, own_out, ours, same, flags = own_pass(
        near_moves + far_moves, sub_count, shards, table, queries, all_keys, all_values
    )
    return pl.pallas_call(
        merge_kernel,
        out_shape=(
            jax.ShapeDtypeStruct(own_out.shape, jnp.float32),
            jax.ShapeDtypeStruct(queries.shape, jnp.float32),
        ),
        in_specs=[VMEM, VMEM, VMEM, VMEM, VMEM, HBM],
        out_specs=(VMEM, HBM),
        input_output_aliases={4: 0, 5: 1},
        scratch_shapes=[
            pltpu.SMEM((shards,), jnp.int32),
            pltpu.SemaphoreType.DMA(()),
            pltpu.SemaphoreType.DMA((shards,)),
        ],
        compiler_params=PARAMS,
        name="merge",
    )(flags, answers, ours, same, own_out, base)[1]


def solution(mesh):
    in_specs = (
        P("ctx", "sub", None),
        P("ctx", "sub", None),
        P("ctx", "sub", None),
        P("ctx", None, None),
    )
    out_specs = P("ctx", "sub", None)

    return jax.shard_map(
        on_device, mesh=mesh, in_specs=in_specs, out_specs=out_specs, check_vma=False
    )
```
